32 devices in a mesh: zero: 4 (over x, core), width: 8 (over z, y).
Axes of the slice: x: 2, y: 2, z: 4, core: 2. Of those that a mesh axis runs over, the one named last changes fastest.
Arguments:
- weight_query: float32 [8192, 8192], P('zero', 'width'), may hold values from -0.09375 to 0.09375
- smooth_query: float32 [8192, 8192], P('zero', 'width'), may hold values from -0.0625 to 0.0625
- weight_key: float32 [8192, 512], P('zero', 'width'), may hold values from -0.09375 to 0.09375
- smooth_key: float32 [8192, 512], P('zero', 'width'), may hold values from -0.0625 to 0.0625
- weight_value: float32 [8192, 512], P('zero', 'width'), may hold values from -0.09375 to 0.09375
- smooth_value: float32 [8192, 512], P('zero', 'width'), may hold values from -0.0625 to 0.0625
- norm_train: float32 [8192], P(('zero', 'width')), may hold values from 0.25 to 1.75
- norm_step: float32 [8192], P(('zero', 'width')), may hold values from -0.3 to 0.3
Outputs:
- final_query: bfloat16 [8192, 8192], P(None, 'width')
- final_key: bfloat16 [8192, 512], P(None, 'width')
- final_value: bfloat16 [8192, 512], P(None, 'width')
- factor_query: float32 [8192], P('width')
- factor_key: float32 [512], P('width')
- factor_value: float32 [512], P('width')
- serve_norm: bfloat16 [8192], replicated
- result_query: float32 [8192, 8192], P('zero', 'width')
- result_key: float32 [8192, 512], P('zero', 'width')
- result_value: float32 [8192, 512], P('zero', 'width')
The draws below stay inside these ranges and needn't reach their ends.
All inputs are finite; a program needn't handle non-finite values. Where the reference program divides by a largest or mean magnitude, that divisor is 1e-20 or more.
Results may differ from the reference program's by a relative error of at most 0.001.
Values may be sent and summed in bfloat16 or wider, within the bound.
No kernel may reach another device: no remote copies, remote signals or barrier semaphores. Data moves between devices by JAX's collectives and lax.ppermute only.
A program may use at most 128 MiB of HBM per device.

```python
import jax
import jax.numpy as jnp

D_MODEL = 8192
Q_DIM = 8192
KV_DIM = 512


def with_spikes(array, stream_key, source, target, shards_of, factor):
    owner, partner = [(jnp.arange(array.shape[position]) // (array.shape[position] // shards_of)).reshape([-1 if axis == position else 1 for axis in range(array.ndim)]) for position in (source, target)]
    chosen = jax.random.permutation(stream_key, shards_of)[partner]
    strong = (owner == chosen) | (owner == (partner + shards_of // 2) % shards_of)
    return jnp.where(strong, factor * array, array)


def block_scale(own_key, dims, shards, least, high):
    level, own = 1.0, jax.random.fold_in(own_key, 6)
    for axis_at, shards_of in shards:
        draws = jnp.exp(jax.random.uniform(jax.random.fold_in(own, axis_at), (shards_of,), jnp.float32, least / len(shards), high / len(shards)))
        level = level * jnp.repeat(draws, dims[axis_at] // shards_of).reshape([-1 if axis == axis_at else 1 for axis in range(len(dims))])
    return level


def normal_values(stream_key, extent, spread, limit, pieces=(), dtype=jnp.bfloat16):
    values = jax.random.normal(stream_key, extent, jnp.float32) * spread
    if len(pieces) > 0:
        values = block_scale(stream_key, extent, pieces, -0.22, 0.18) * values
    return jnp.clip(values, min=-limit, max=limit).astype(dtype)


def gaussian_with(rng, shape, width, most, cuts, heavy, kind=jnp.bfloat16):
    drawn = width * jax.random.normal(rng, shape, jnp.float32)
    if cuts:
        drawn = drawn * block_scale(rng, shape, cuts, -0.22, 0.18)
    return jnp.clip(with_spikes(drawn, jax.random.fold_in(rng, 3), *heavy), -most, most).astype(kind)


def setup_inputs(seed: int = 0) -> dict:
    key_list = jax.random.split(jax.random.key(seed), 9)
    return {
        "weight_query": gaussian_with(key_list[0], (D_MODEL, Q_DIM), D_MODEL ** -0.5, 0.09375, ((0, 4), (1, 8)), (0, 1, 8, 2.0), jnp.float32),
        "smooth_query": normal_values(key_list[1], (D_MODEL, Q_DIM), D_MODEL ** -0.5, 0.0625, ((0, 4), (1, 8)), jnp.float32),
        "weight_key": gaussian_with(key_list[2], (D_MODEL, KV_DIM), D_MODEL ** -0.5, 0.09375, ((0, 4), (1, 8)), (0, 1, 8, 2.0), jnp.float32),
        "smooth_key": normal_values(key_list[3], (D_MODEL, KV_DIM), D_MODEL ** -0.5, 0.0625, ((0, 4), (1, 8)), jnp.float32),
        "weight_value": gaussian_with(key_list[4], (D_MODEL, KV_DIM), D_MODEL ** -0.5, 0.09375, ((0, 4), (1, 8)), (0, 1, 8, 2.0), jnp.float32),
        "smooth_value": normal_values(key_list[5], (D_MODEL, KV_DIM), D_MODEL ** -0.5, 0.0625, ((0, 4), (1, 8)), jnp.float32),
        "norm_train": jnp.clip(1.0 + 0.15 * jax.random.normal(key_list[6], (D_MODEL,), jnp.float32), 0.25, 1.75),
        "norm_step": jnp.clip(jax.random.uniform(key_list[7], (D_MODEL,), jnp.float32, -0.3, 0.3) * block_scale(key_list[7], (D_MODEL,), ((0, 32),), -0.4, 0.0), -0.3, 0.3),
    }


keep_rate = 0.7


def reference(weight_query, smooth_query, weight_key, smooth_key, weight_value, smooth_value, norm_train, norm_step):
    result_query = keep_rate * smooth_query + (1.0 - keep_rate) * weight_query
    result_key = keep_rate * smooth_key + (1.0 - keep_rate) * weight_key
    result_value = keep_rate * smooth_value + (1.0 - keep_rate) * weight_value
    factor_query = jnp.sum(jnp.abs(result_query), axis=0) / D_MODEL
    final_query = (result_query / factor_query).astype(jnp.bfloat16)
    factor_key = jnp.sum(jnp.abs(result_key), axis=0) / D_MODEL
    final_key = (result_key / factor_key).astype(jnp.bfloat16)
    factor_value = jnp.sum(jnp.abs(result_value), axis=0) / D_MODEL
    final_value = (result_value / factor_value).astype(jnp.bfloat16)
    serve_norm = (norm_train + norm_step).astype(jnp.bfloat16)
    return final_query, final_key, final_value, factor_query, factor_key, factor_value, serve_norm, result_query, result_key, result_value
```

```python
import functools

import jax
import jax.numpy as jnp
from jax import lax
from jax.experimental import pallas as pl
from jax.experimental.pallas import tpu as pltpu
from jax.sharding import PartitionSpec as P

KEEP = 0.7
LANES = 128

VMEM = pl.BlockSpec(memory_space=pltpu.VMEM)
SMEM = pl.BlockSpec(memory_space=pltpu.SMEM)
HBM = pl.BlockSpec(memory_space=pl.ANY)


def cost(flops, bytes_accessed):
    return pl.CostEstimate(flops=flops, bytes_accessed=bytes_accessed, transcendentals=0)


def round_up(value, step):
    return -(-value // step) * step


def average(smooth, weight):
    return KEEP * smooth + (1.0 - KEEP) * weight


def lane_sum(block):
    total = block[:, :LANES]
    for at in range(LANES, block.shape[1], LANES):
        total = total + block[:, at : at + LANES]
    return total


def average_kernel(
    places, wq, sq, wk, sk, wv, sv, nt, ns, rq, rk, rv, message, sum_q, sum_kv
):
    step, steps = pl.program_id(0), pl.num_programs(0)
    heads = wk.shape[0]

    @pl.when(step == 0)
    def _():
        sum_q[...] = jnp.zeros_like(sum_q)
        sum_kv[...] = jnp.zeros_like(sum_kv)

    new_q = average(sq[...], wq[...])
    rq[...] = new_q
    rows, width = new_q.shape
    sum_q[...] += jnp.sum(jnp.abs(new_q).reshape(rows // 8, 8, width), axis=0)
    for at, (w, s, r) in enumerate(((wk, sk, rk), (wv, sv, rv))):
        new = average(s[...], w[...])
        r[...] = new
        sum_kv[at * heads : (at + 1) * heads, :] += lane_sum(jnp.abs(new))

    @pl.when(step == steps - 1)
    def _():
        place_kv, place_norm = places
        message[...] = jnp.zeros_like(message)
        message[:, :width] = jnp.sum(sum_q[...], axis=0, keepdims=True)
        message[:, place_kv : place_kv + 2 * heads] = jnp.sum(
            sum_kv[...].T, axis=0, keepdims=True
        )
        gain = (nt[...] + ns[...]).astype(jnp.bfloat16)
        message[:, place_norm : place_norm + gain.shape[1]] = gain.astype(jnp.float32)


def first_kernel(places, sizes, rows_all, me, rq, *refs):
    n = len(refs) - 6
    messages, (own, inv_q, inv_kv, factor_q, factor_kv, norms) = refs[:n], refs[n:]
    place_kv, place_norm = places
    width, heads, gain = sizes
    pieces = [m[...] for m in messages]
    for distance, piece in enumerate(pieces):
        norms[pl.ds(me[0] ^ distance, 1), :] = piece[:, place_norm : place_norm + gain]
    while len(pieces) > 1:
        pieces = [a + b for a, b in zip(pieces[::2], pieces[1::2])]
    total = pieces[0] / rows_all
    factor_q[...] = total[:, :width]
    of_kv = total[:, place_kv : place_kv + 2 * heads]
    factor_kv[...] = of_kv
    inv = 1.0 / total[:, :width]
    inv_q[...] = inv
    inv_kv[...] = jnp.broadcast_to(1.0 / of_kv, (LANES, 2 * heads)).T
    own[...] = (rq[...] * inv).astype(jnp.bfloat16)


def scale_kernel(rq, inv, own):
    own[...] = (rq[...] * inv[...]).astype(jnp.bfloat16)


def scale_kv_kernel(rk, rv, inv, own):
    heads, rows = rk.shape
    for at, r in enumerate((rk, rv)):
        scale = inv[at * heads : (at + 1) * heads, :]
        for lane in range(0, rows, LANES):
            own[at * heads : (at + 1) * heads, lane : lane + LANES] = (
                r[:, lane : lane + LANES] * scale
            ).astype(jnp.bfloat16)


def place_kernel(plan, rows, aliased, me, *refs):
    pieces, (out, sems) = refs[: len(plan)], refs[-2:]
    copies = []
    for at, (piece, (distance, first)) in enumerate(zip(pieces, plan)):
        start = pl.multiple_of((me[0] ^ distance) * rows + first, 16)
        copies.append(
            pltpu.make_async_copy(
                piece, out.at[pl.ds(start, piece.shape[0]), :], sems.at[at]
            )
        )
    for copy in copies:
        copy.start()
    for copy in copies:
        copy.wait()


def place_kv_kernel(me, *refs):
    pieces, (out_k, out_v, sems) = refs[:-3], refs[-3:]
    heads, rows = pieces[0].shape[0] // 2, pieces[0].shape[1]
    copies = []
    for distance, piece in enumerate(pieces):
        start = pl.multiple_of((me[0] ^ distance) * rows, LANES)
        for at, out in enumerate((out_k, out_v)):
            copies.append(
                pltpu.make_async_copy(
                    piece.at[at * heads : (at + 1) * heads, :],
                    out.at[:, pl.ds(start, rows)],
                    sems.at[2 * distance + at],
                )
            )
    for copy in copies:
        copy.start()
    for copy in copies:
        copy.wait()


def place(me, rows, plan, pieces, out_shape, out=None):
    count = len(plan)
    moved = sum(p.size for p in pieces) * 2
    return pl.pallas_call(
        functools.partial(place_kernel, plan, rows, out is not None),
        out_shape=out_shape,
        in_specs=[SMEM] + [VMEM] * count + ([HBM] if out is not None else []),
        out_specs=HBM,
        scratch_shapes=[pltpu.SemaphoreType.DMA((count,))],
        input_output_aliases={count + 1: 0} if out is not None else {},
        cost_estimate=cost(moved * 8, 2 * moved),
    )(me, *pieces, *(() if out is None else (out,)))


def on_device(n, groups, wq, sq, wk, sk, wv, sv, norm_train, norm_step):
    rows, width = wq.shape
    heads = wk.shape[1]
    gain = norm_train.shape[0]
    me = lax.axis_index("zero").astype(jnp.int32).reshape(1)

    def swap(array, distance, axis="zero", size=n):
        return lax.ppermute(array, axis, [(i, i ^ distance) for i in range(size)])

    def gather(piece):
        found = [piece, swap(piece, 1)]
        for distance in range(2, n, 2):
            far = swap(piece, distance)
            found += [far, swap(far, 1)]
        return found

    place_kv = round_up(width, LANES)
    place_norm = place_kv + round_up(2 * heads, LANES)
    places = (place_kv, place_norm)
    length = place_norm + round_up(gain, LANES)
    block = min(rows, 256)
    of_q = pl.BlockSpec((block, width), lambda i: (i, 0))
    of_kv = pl.BlockSpec((heads, block), lambda i: (0, i))
    once = lambda shape: pl.BlockSpec(shape, lambda i: (0, 0))
    rq, rk, rv, message = pl.pallas_call(
        functools.partial(average_kernel, places),
        grid=(rows // block,),
        out_shape=(
            jax.ShapeDtypeStruct((rows, width), jnp.float32),
            jax.ShapeDtypeStruct((heads, rows), jnp.float32),
            jax.ShapeDtypeStruct((heads, rows), jnp.float32),
            jax.ShapeDtypeStruct((1, length), jnp.float32),
        ),
        in_specs=[of_q] * 2 + [of_kv] * 4 + [once((1, gain))] * 2,
        out_specs=[of_q, of_kv, of_kv, once((1, length))],
        scratch_shapes=[
            pltpu.VMEM((8, width), jnp.float32),
            pltpu.VMEM((2 * heads, LANES), jnp.float32),
        ],
        cost_estimate=cost(rows * (width + 2 * heads) * 5, rows * (width + 2 * heads) * 12),
    )(wq, sq, wk.T, sk.T, wv.T, sv.T, norm_train[None], norm_step[None])

    messages = gather(message)

    unit = rows // 16
    cuts = [1, 1] + [2] * 6 + [1, 1]
    firsts = [sum(cuts[:at]) for at in range(len(cuts))]
    size = cuts[0] * unit
    own0, inv_q, inv_kv, factor_q, factor_kv, norms = pl.pallas_call(
        functools.partial(first_kernel, places, (width, heads, gain), n * rows),
        grid=(1,),
        out_shape=(
            jax.ShapeDtypeStruct((size, width), jnp.bfloat16),
            jax.ShapeDtypeStruct((1, width), jnp.float32),
            jax.ShapeDtypeStruct((2 * heads, LANES), jnp.float32),
            jax.ShapeDtypeStruct((1, width), jnp.float32),
            jax.ShapeDtypeStruct((1, 2 * heads), jnp.float32),
            jax.ShapeDtypeStruct((n, gain), jnp.float32),
        ),
        in_specs=[SMEM, pl.BlockSpec((size, width), lambda i: (0, 0))]
        + [once((1, length))] * n,
        out_specs=[
            once((size, width)),
            once((1, width)),
            once((2 * heads, LANES)),
            once((1, width)),
            once((1, 2 * heads)),
            once((n, gain)),
        ],
        cost_estimate=cost(size * width * 4, size * width * 6),
    )(me, rq, *messages)

    def scaled(first, size):
        parts = 2
        sub = size // parts
        at = first * parts // (size // unit)
        return pl.pallas_call(
            scale_kernel,
            grid=(parts,),
            out_shape=jax.ShapeDtypeStruct((size, width), jnp.bfloat16),
            in_specs=[
                pl.BlockSpec((sub, width), lambda i: (at + i, 0)),
                pl.BlockSpec((1, width), lambda i: (0, 0)),
            ],
            out_specs=pl.BlockSpec((sub, width), lambda i: (i, 0)),
            cost_estimate=cost(size * width * 4, size * width * 6),
        )(rq, inv_q)

    own = [own0] + [scaled(f, c * unit) for f, c in zip(firsts[1:], cuts[1:])]
    own_kv = pl.pallas_call(
        scale_kv_kernel,
        out_shape=jax.ShapeDtypeStruct((2 * heads, rows), jnp.bfloat16),
        in_specs=[VMEM] * 3,
        out_specs=VMEM,
        cost_estimate=cost(2 * heads * rows * 4, 2 * heads * rows * 6),
    )(rk, rv, inv_kv)

    found = [gather(piece) for piece in own[:-1]]
    found_kv = gather(own_kv)
    found.append(gather(own[-1]))

    whole = jax.ShapeDtypeStruct((n * rows, width), jnp.bfloat16)
    final_q = None
    for distances in [(0, 1)] + [(d, d + 1) for d in range(2, n, 2)]:
        if distances == (0, 1):
            plan = [(d, f * unit) for f in firsts for d in distances]
            pieces = [piece[d] for piece in found for d in distances]
            final_q = place(me, rows, plan, pieces, whole)
        else:
            for f, piece in zip(firsts, found):
                plan = [(d, f * unit) for d in distances]
                final_q = place(me, rows, plan, [piece[d] for d in distances], whole, final_q)

    moved = n * own_kv.size * 2
    final_k, final_v = pl.pallas_call(
        place_kv_kernel,
        out_shape=(jax.ShapeDtypeStruct((heads, n * rows), jnp.bfloat16),) * 2,
        in_specs=[SMEM] + [VMEM] * n,
        out_specs=[HBM] * 2,
        scratch_shapes=[pltpu.SemaphoreType.DMA((2 * n,))],
        cost_estimate=cost(moved * 8, 2 * moved),
    )(me, *found_kv)

    gains = norms.astype(jnp.bfloat16).reshape(n, 1, gain)
    spot = lax.axis_index("width")
    bit = 1
    while bit < groups:
        other = swap(gains, bit, "width", groups)
        low = (spot & bit) == 0
        gains = jnp.concatenate(
            [jnp.where(low, gains, other), jnp.where(low, other, gains)], axis=1
        )
        bit *= 2

    return (
        final_q,
        final_k.T,
        final_v.T,
        factor_q.reshape(width),
        factor_kv[0, :heads],
        factor_kv[0, heads:],
        gains.reshape(n * groups * gain),
        rq,
        rk.T,
        rv.T,
    )


def solution(mesh):
    split, columns, lone = P("zero", "width"), P(None, "width"), P("width")
    vector = P(("zero", "width"))
    return jax.shard_map(
        functools.partial(on_device, mesh.shape["zero"], mesh.shape["width"]),
        mesh=mesh,
        in_specs=(split,) * 6 + (vector,) * 2,
        out_specs=(columns,) * 3 + (lone,) * 3 + (P(),) + (split,) * 3,
        check_vma=False,
    )
```

```python
import functools

import jax
import jax.numpy as jnp
from jax import lax
from jax.experimental import pallas as pl
from jax.experimental.pallas import tpu as pltpu
from jax.sharding import PartitionSpec as P


KEEP = 0.7
LANES = 128

VMEM = pl.BlockSpec(memory_space=pltpu.VMEM)
SMEM = pl.BlockSpec(memory_space=pltpu.SMEM)
HBM = pl.BlockSpec(memory_space=pl.ANY)


def cost(flops, bytes_accessed):
    return pl.CostEstimate(flops=flops, bytes_accessed=bytes_accessed, transcendentals=0)


def round_up(value, step):
    return -(-value // step) * step


def average(smooth, weight):
    return KEEP * smooth + (1.0 - KEEP) * weight


def lane_sum(block):
    total = block[:, :LANES]
    for at in range(LANES, block.shape[1], LANES):
        total = total + block[:, at : at + LANES]
    return total


def row_sum(block):
    return jnp.sum(block.reshape(block.shape[0] // 8, 8, block.shape[1]), axis=0)


def narrow_kernel(places, wq, sq, wk, sk, wv, sv, nt, ns, rk, rv, message, sum_q, sum_kv):
    step, steps = pl.program_id(0), pl.num_programs(0)
    heads = wk.shape[0]

    @pl.when(step == 0)
    def _():
        sum_q[...] = jnp.zeros_like(sum_q)
        sum_kv[...] = jnp.zeros_like(sum_kv)

    sum_q[...] += row_sum(jnp.abs(average(sq[...], wq[...])))
    for at, (w, s, r) in enumerate(((wk, sk, rk), (wv, sv, rv))):
        new = average(s[...], w[...])
        r[...] = new
        sum_kv[at * heads : (at + 1) * heads, :] += lane_sum(jnp.abs(new))

    @pl.when(step == steps - 1)
    def _():
        place_kv, place_norm = places
        message[...] = jnp.zeros_like(message)
        message[:, : sum_q.shape[1]] = jnp.sum(sum_q[...], axis=0, keepdims=True)
        message[:, place_kv : place_kv + 2 * heads] = jnp.sum(
            sum_kv[...].T, axis=0, keepdims=True
        )
        gain = (nt[...] + ns[...]).astype(jnp.bfloat16)
        message[:, place_norm : place_norm + gain.shape[1]] = gain.astype(jnp.float32)


def tree(pieces):
    while len(pieces) > 1:
        pieces = [a + b for a, b in zip(pieces[::2], pieces[1::2])]
    return pieces[0]


def first_kernel(places, columns, gain, count, me, rk, rv, *refs):
    n = len(refs) - 5
    messages, (own, inv_q, factor_k, factor_v, norms) = refs[:n], refs[n:]
    place_kv, place_norm = places
    heads = rk.shape[0]
    pieces = [m[...] for m in messages]
    for distance, piece in enumerate(pieces):
        norms[pl.ds(me[0] ^ distance, 1), :] = piece[:, place_norm : place_norm + gain]
    total = tree(pieces) / count
    inv_q[...] = 1.0 / total[:, :columns]
    of_kv = total[:, place_kv : place_kv + 2 * heads]
    factor_k[...] = of_kv[:, :heads]
    factor_v[...] = of_kv[:, heads:]
    inv = jnp.broadcast_to(1.0 / of_kv, (LANES, 2 * heads)).T
    for at, r in enumerate((rk, rv)):
        scale = inv[at * heads : (at + 1) * heads, :]
        for lane in range(0, rk.shape[1], LANES):
            own[at * heads : (at + 1) * heads, lane : lane + LANES] = (
                r[:, lane : lane + LANES] * scale
            ).astype(jnp.bfloat16)


def second_kernel(wq, sq, inv, *owns):
    first = 0
    for own in owns:
        rows = pl.ds(first, own.shape[0])
        own[...] = (average(sq[rows, :], wq[rows, :]) * inv[...]).astype(jnp.bfloat16)
        first += own.shape[0]


def average_kernel(wq, sq, rq, message, sum_q):
    step, steps = pl.program_id(0), pl.num_programs(0)

    @pl.when(step == 0)
    def _():
        sum_q[...] = jnp.zeros_like(sum_q)

    new = average(sq[...], wq[...])
    rq[...] = new
    sum_q[...] += row_sum(jnp.abs(new))

    @pl.when(step == steps - 1)
    def _():
        message[...] = jnp.sum(sum_q[...], axis=0, keepdims=True)


def third_kernel(columns, count, rq, *refs):
    messages, (own, inv, factor) = refs[:-3], refs[-3:]
    total = tree([m[...] for m in messages]) / count
    factor[...] = total
    scale = 1.0 / total[:, columns:]
    inv[...] = scale
    own[...] = (rq[:, columns:] * scale).astype(jnp.bfloat16)


def fourth_kernel(inv, *refs):
    half = len(refs) // 2
    for source, own in zip(refs[:half], refs[half:]):
        columns = source.shape[1] - own.shape[1]
        own[...] = (source[:, columns:] * inv[...]).astype(jnp.bfloat16)


def place_kernel(plan, rows, kv, whole, me, *refs):
    pieces, refs = refs[: len(plan)], refs[len(plan) :]
    kv_pieces, refs = refs[:kv], refs[kv + (1 if whole else 0) :]
    out, kv_outs, sems = refs[0], refs[1:-1], refs[-1]
    copies = []

    def move(source, target):
        copies.append(pltpu.make_async_copy(source, target, sems.at[len(copies)]))
        copies[-1].start()

    for piece, (distance, first, column) in zip(pieces, plan):
        start = pl.multiple_of((me[0] ^ distance) * rows + first, 16)
        move(piece, out.at[pl.ds(start, piece.shape[0]), pl.ds(column, piece.shape[1])])
    for distance, piece in enumerate(kv_pieces):
        heads = piece.shape[0] // 2
        start = pl.multiple_of((me[0] ^ distance) * rows, LANES)
        for at, target in enumerate(kv_outs):
            move(
                piece.at[at * heads : (at + 1) * heads, :],
                target.at[:, pl.ds(start, rows)],
            )
    for copy in copies:
        copy.wait()


CUTS = (4,) * 7 + (2, 1, 1)


def on_device(n, groups, wq, sq, wk, sk, wv, sv, norm_train, norm_step):
    rows, width = wq.shape
    heads = wk.shape[1]
    gain = norm_train.shape[0]
    f32, bf16 = jnp.float32, jnp.bfloat16
    shaped = jax.ShapeDtypeStruct
    me = lax.axis_index("zero").astype(jnp.int32).reshape(1)

    def swap(array, distance, axis="zero", size=n):
        return lax.ppermute(array, axis, [(i, i ^ distance) for i in range(size)])

    def gather(piece):
        found = [piece, swap(piece, 1)]
        for distance in range(2, n, 2):
            far = swap(piece, distance)
            found += [far, swap(far, 1)]
        return found

    def exchange(piece):
        found = [piece]
        for distance in range(1, n):
            found.append(swap(piece, distance))
        return found

    once = lambda shape: pl.BlockSpec(shape, lambda i: (0, 0))
    full = lambda a: once(a.shape)

    columns = max(LANES, width // 8)
    place_kv = columns
    place_norm = place_kv + round_up(2 * heads, LANES)
    places = (place_kv, place_norm)
    length = place_norm + round_up(gain, LANES)
    block = rows // 4
    of_q = pl.BlockSpec((block, columns), lambda i: (i, 0))
    of_kv = pl.BlockSpec((heads, block), lambda i: (0, i))
    rk, rv, message = pl.pallas_call(
        functools.partial(narrow_kernel, places),
        grid=(rows // block,),
        out_shape=(
            shaped((heads, rows), f32),
            shaped((heads, rows), f32),
            shaped((1, length), f32),
        ),
        in_specs=[of_q] * 2 + [of_kv] * 4 + [once((1, gain))] * 2,
        out_specs=[of_kv, of_kv, once((1, length))],
        scratch_shapes=[pltpu.VMEM((8, columns), f32), pltpu.VMEM((2 * heads, LANES), f32)],
        cost_estimate=cost(rows * 2 * heads * 8, rows * 2 * heads * 16),
        name="narrow",
    )(wq, sq, wk.T, sk.T, wv.T, sv.T, norm_train[None], norm_step[None])
    messages = exchange(message)
    own_kv, inv_a, factor_k, factor_v, norms = pl.pallas_call(
        functools.partial(first_kernel, places, columns, gain, n * rows),
        grid=(1,),
        out_shape=(
            shaped((2 * heads, rows), bf16),
            shaped((1, columns), f32),
            shaped((1, heads), f32),
            shaped((1, heads), f32),
            shaped((n, gain), f32),
        ),
        in_specs=[SMEM] + [full(rk)] * 2 + [full(message)] * n,
        out_specs=[
            once((2 * heads, rows)),
            once((1, columns)),
            once((1, heads)),
            once((1, heads)),
            once((n, gain)),
        ],
        cost_estimate=cost(rows * heads * 8, rows * heads * 12),
        name="first",
    )(me, rk, rv, *messages)
    part = shaped((rows // 2, columns), bf16)
    own_a = pl.pallas_call(
        second_kernel,
        grid=(1,),
        out_shape=(part,) * 2,
        in_specs=[once((rows, columns))] * 2 + [full(inv_a)],
        out_specs=[full(part)] * 2,
        cost_estimate=cost(rows * columns * 8, rows * columns * 10),
        name="second",
    )(wq, sq, inv_a)
    found_kv = gather(own_kv)
    found_a = [gather(piece) for piece in own_a]

    block = min(rows, 256)
    of_q = pl.BlockSpec((block, width), lambda i: (i, 0))
    rq, message_q = pl.pallas_call(
        average_kernel,
        grid=(rows // block,),
        out_shape=(shaped((rows, width), f32), shaped((1, width), f32)),
        in_specs=[of_q] * 2,
        out_specs=[of_q, once((1, width))],
        scratch_shapes=[pltpu.VMEM((8, width), f32)],
        cost_estimate=cost(rows * width * 8, rows * width * 12),
        name="average",
    )(wq, sq)
    messages_q = exchange(message_q)

    unit = rows // sum(CUTS)
    firsts = [sum(CUTS[:at]) for at in range(len(CUTS))]
    rest = width - columns
    rows_of = lambda at: pl.BlockSpec(
        (CUTS[at] * unit, width), lambda i: (firsts[at] // CUTS[at], 0)
    )
    narrow = [shaped((c * unit, rest), bf16) for c in CUTS]
    own0, inv, factor_q = pl.pallas_call(
        functools.partial(third_kernel, columns, n * rows),
        grid=(1,),
        out_shape=(narrow[0], shaped((1, rest), f32), shaped((1, width), f32)),
        in_specs=[rows_of(0)] + [full(message_q)] * n,
        out_specs=[full(narrow[0]), once((1, rest)), once((1, width))],
        cost_estimate=cost(narrow[0].size * 8, narrow[0].size * 6),
        name="third",
    )(rq, *messages_q)
    others = range(1, len(CUTS))
    owns = pl.pallas_call(
        fourth_kernel,
        grid=(1,),
        out_shape=narrow[1:],
        in_specs=[full(inv)] + [rows_of(at) for at in others],
        out_specs=[full(narrow[at]) for at in others],
        cost_estimate=cost(rows * rest * 8, rows * rest * 6),
        name="fourth",
    )(inv, *[rq for _ in others])
    found = [gather(piece) for piece in [own0, *owns]]

    whole = shaped((n * rows, width), bf16)
    whole_kv = shaped((heads, n * rows), bf16)

    def place(jobs, kv=(), final=None):
        pieces = [job[0] for job in jobs]
        operands = [*pieces, *kv]
        moved = sum(p.size for p in operands) * 2
        return pl.pallas_call(
            functools.partial(
                place_kernel, [job[1:] for job in jobs], rows, len(kv), final is not None
            ),
            grid=(1,),
            out_shape=[whole] + [whole_kv] * (2 if kv else 0),
            in_specs=[SMEM]
            + [full(p) for p in operands]
            + ([HBM] if final is not None else []),
            out_specs=[HBM] * (3 if kv else 1),
            scratch_shapes=[pltpu.SemaphoreType.DMA((len(jobs) + 2 * len(kv),))],
            input_output_aliases={} if final is None else {1 + len(operands): 0},
            cost_estimate=cost(moved * 4, 2 * moved),
        )(me, *operands, *(() if final is None else (final,)))

    def jobs(chunks, distances):
        return [
            (found[at][d], d, firsts[at] * unit, columns) for at in chunks for d in distances
        ]

    near, far = range(2), range(2, n)
    final_q, final_k, final_v = place(
        [(found_a[at][d], d, at * rows // 2, 0) for at in range(2) for d in range(n)], found_kv
    )
    for chunks, distances in (
        (range(len(CUTS)), near),
        ((0, 1, 2), far),
        ((3, 4), far),
        ((5,), far),
        ((6,), far),
        ((7,), far),
        ((8, 9), far),
    ):
        (final_q,) = place(jobs(chunks, distances), (), final_q)

    gains = norms.astype(jnp.bfloat16).reshape(n, 1, gain)
    spot = lax.axis_index("width")
    bit = 1
    while bit < groups:
        other = swap(gains, bit, "width", groups)
        low = (spot & bit) == 0
        gains = jnp.concatenate(
            [jnp.where(low, gains, other), jnp.where(low, other, gains)], axis=1
        )
        bit *= 2

    return (
        final_q,
        final_k.T,
        final_v.T,
        factor_q.reshape(width),
        factor_k.reshape(heads),
        factor_v.reshape(heads),
        gains.reshape(n * groups * gain),
        rq,
        rk.T,
        rv.T,
    )


def solution(mesh):
    split, columns, lone = P("zero", "width"), P(None, "width"), P("width")
    vector = P(("zero", "width"))
    n = mesh.shape["zero"]

    def body(*args):
        return on_device(n, mesh.shape["width"], *args)

    return jax.shard_map(
        body,
        mesh=mesh,
        in_specs=(split,) * 6 + (vector,) * 2,
        out_specs=(columns,) * 3 + (lone,) * 3 + (P(),) + (split,) * 3,
        check_vma=False,
    )
```

```python
import functools

import jax
import jax.numpy as jnp
from jax import lax
from jax.experimental import pallas as pl
from jax.experimental.pallas import tpu as pltpu
from jax.sharding import PartitionSpec as P


KEEP = 0.7
LANES = 128
GRANT_KIB = 60 * 1024

VMEM = pl.BlockSpec(memory_space=pltpu.VMEM)
SMEM = pl.BlockSpec(memory_space=pltpu.SMEM)
HBM = pl.BlockSpec(memory_space=pl.ANY)


def cost(flops, bytes_accessed):
    return pl.CostEstimate(flops=flops, bytes_accessed=bytes_accessed, transcendentals=0)


def leaving(kibibytes):
    return pltpu.CompilerParams(vmem_limit_bytes=(GRANT_KIB - kibibytes) << 10)


def round_up(value, step):
    return -(-value // step) * step


def average(smooth, weight):
    return KEEP * smooth + (1.0 - KEEP) * weight


def lane_sum(block):
    total = block[:, :LANES]
    for at in range(LANES, block.shape[1], LANES):
        total = total + block[:, at : at + LANES]
    return total


def row_sum(block):
    return jnp.sum(block.reshape(block.shape[0] // 8, 8, block.shape[1]), axis=0)


def load(sources, buffers, parts, sems):
    copies = []
    for at in range(parts):
        copies.append([])
        for source, buffer in zip(sources, buffers):
            step = buffer.shape[0] // parts
            rows = pl.ds(at * step, step)
            slot = sems.at[at * len(sources) + len(copies[-1])]
            copies[-1].append(
                pltpu.make_async_copy(
                    source.at[rows, pl.ds(0, buffer.shape[1])], buffer.at[rows, :], slot
                )
            )
            copies[-1][-1].start()

    def wait(at):
        for copy in copies[at]:
            copy.wait()

    return wait


PARTS = 4


def narrow_kernel(places, wq, sq, wk, sk, wv, sv, nt, ns, rk, rv, early, message, *refs):
    *buffers, gain_a, gain_b, note, sum_kv, in_kv, in_q, in_gain, outs = refs
    of_kv, of_q = buffers[:4], buffers[4:]
    place_kv, place_norm = places
    heads, rows = of_kv[0].shape
    wait_kv = load((wk, sk, wv, sv), of_kv, PARTS, in_kv)
    wait_gain = load((nt, ns), (gain_a, gain_b), 1, in_gain)
    wait_q = load((wq, sq), of_q, PARTS, in_q)
    step = heads // PARTS
    writes = []

    def write(source, target):
        writes.append(pltpu.make_async_copy(source, target, outs.at[len(writes)]))
        writes[-1].start()

    for part in range(PARTS):
        wait_kv(part)
        at = pl.ds(part * step, step)
        for which, (w, s, r) in enumerate(((of_kv[0], of_kv[1], rk), (of_kv[2], of_kv[3], rv))):
            new = average(s[at, :], w[at, :])
            sum_kv[which * heads + part * step : which * heads + (part + 1) * step, :] = (
                lane_sum(jnp.abs(new))
            )
            s[at, :] = new
            write(s.at[at, :], r.at[at, :])
            if which == 0:
                write(s.at[at, pl.ds(0, early.shape[1])], early.at[at, :])
    total = jnp.zeros((8, of_q[0].shape[1]), jnp.float32)
    step = rows // PARTS
    for part in range(PARTS):
        wait_q(part)
        at = pl.ds(part * step, step)
        total = total + row_sum(jnp.abs(average(of_q[1][at, :], of_q[0][at, :])))
    note[...] = jnp.zeros_like(note)
    note[:, : total.shape[1]] = jnp.sum(total, axis=0, keepdims=True)
    note[:, place_kv : place_kv + 2 * heads] = jnp.sum(
        sum_kv[...].T, axis=0, keepdims=True
    )
    wait_gain(0)
    gain = (gain_a[...] + gain_b[...]).astype(jnp.bfloat16)
    note[:, place_norm : place_norm + gain.shape[1]] = gain.astype(jnp.float32)
    write(note, message)
    for copy in writes:
        copy.wait()


def tree(pieces):
    while len(pieces) > 1:
        pieces = [a + b for a, b in zip(pieces[::2], pieces[1::2])]
    return pieces[0]


def first_kernel(places, gain, count, me, rk, rv, wq, sq, *refs):
    n = len(refs) - 7
    messages, (own, own_a, own_b, inv_k, factor_k, factor_v, norms) = refs[:n], refs[n:]
    place_kv, place_norm = places
    heads, rows = rk.shape
    pieces = [m[...] for m in messages]
    for distance, piece in enumerate(pieces):
        norms[pl.ds(me[0] ^ distance, 1), :] = piece[:, place_norm : place_norm + gain]
    total = tree(pieces) / count
    first = 0
    for part in (own_a, own_b):
        at = pl.ds(first, part.shape[0])
        first += part.shape[0]
        part[...] = (average(sq[at, :], wq[at, :]) / total[:, : part.shape[1]]).astype(
            jnp.bfloat16
        )
    of_kv = total[:, place_kv : place_kv + 2 * heads]
    factor_k[...] = of_kv[:, :heads]
    factor_v[...] = of_kv[:, heads:]
    inv = jnp.broadcast_to(1.0 / of_kv, (LANES, 2 * heads)).T
    inv_k[...] = inv[:heads, :]
    late = 2 * rows - own.shape[1]
    scale_lanes(rk, inv[:heads, :], own, late, 0, rows - late)
    scale_lanes(rv, inv[heads:, :], own, 0, rows - late, rows)


def scale_lanes(source, scale, target, first, to, count):
    for at in range(0, count, LANES):
        target[:, to + at : to + at + LANES] = (
            source[:, first + at : first + at + LANES] * scale
        ).astype(jnp.bfloat16)


def average_kernel(wq, sq, rq, message, w, s, note, in_w, in_s, outs, sent):
    parts = in_w.shape[0]
    step = w.shape[0] // parts

    def copies(at):
        rows = pl.ds(pl.multiple_of(at * step, step), step)
        return (
            pltpu.make_async_copy(wq.at[rows, :], w.at[rows, :], in_w.at[at]),
            pltpu.make_async_copy(sq.at[rows, :], s.at[rows, :], in_s.at[at]),
            pltpu.make_async_copy(s.at[rows, :], rq.at[rows, :], outs.at[at]),
        )

    @pl.loop(0, parts)
    def _(at):
        one, two, _ = copies(at)
        one.start()
        two.start()

    def body(at, total):
        one, two, out = copies(at)
        one.wait()
        two.wait()
        rows = pl.ds(pl.multiple_of(at * step, step), step)
        new = average(s[rows, :], w[rows, :])
        s[rows, :] = new
        out.start()
        return total + row_sum(jnp.abs(new))

    total = lax.fori_loop(0, parts, body, jnp.zeros((8, w.shape[1]), jnp.float32))
    note[...] = jnp.sum(total, axis=0, keepdims=True)
    send = pltpu.make_async_copy(note, message, sent)
    send.start()

    @pl.loop(0, parts)
    def _(at):
        copies(at)[2].wait()

    send.wait()


def third_kernel(columns, count, rq, *refs):
    messages, (own, inv, factor) = refs[:-3], refs[-3:]
    total = tree([m[...] for m in messages]) / count
    factor[...] = total
    scale = 1.0 / total[:, columns:]
    inv[...] = scale
    own[...] = (rq[:, columns:] * scale).astype(jnp.bfloat16)


def fourth_kernel(inv, *refs):
    half = len(refs) // 2
    for source, own in zip(refs[:half], refs[half:]):
        columns = source.shape[1] - own.shape[1]
        own[...] = (source[:, columns:] * inv[...]).astype(jnp.bfloat16)


def place_kernel(plan, rows, unread, me, *refs):
    pieces, refs = refs[: len(plan)], refs[len(plan) + unread :]
    out, sems = refs
    copies = []
    for piece, (distance, first, column) in zip(pieces, plan):
        start = pl.multiple_of((me[0] ^ distance) * rows + first, 16)
        target = out.at[pl.ds(start, piece.shape[0]), pl.ds(column, piece.shape[1])]
        copies.append(pltpu.make_async_copy(piece, target, sems.at[len(copies)]))
        copies[-1].start()
    for copy in copies:
        copy.wait()


def place_kv_kernel(n, me, inv, *refs):
    early, pieces, (out_k, out_v, scaled, sems) = refs[:n], refs[n : 2 * n], refs[2 * n :]
    part = early[0].shape[1]
    rows = (pieces[0].shape[1] + part) // 2
    copies = []

    def move(source, target):
        copies.append(pltpu.make_async_copy(source, target, sems.at[len(copies)]))
        copies[-1].start()

    starts = [pl.multiple_of((me[0] ^ distance) * rows, LANES) for distance in range(n)]
    for start, piece in zip(starts, pieces):
        late = rows - part
        move(piece.at[:, pl.ds(0, late)], out_k.at[:, pl.ds(start + part, late)])
        move(piece.at[:, pl.ds(late, rows)], out_v.at[:, pl.ds(start, rows)])
    for distance, start in enumerate(starts):
        scale_lanes(early[distance], inv[...], scaled.at[distance], 0, 0, part)
        move(scaled.at[distance], out_k.at[:, pl.ds(start, part)])
    for copy in copies:
        copy.wait()


CUTS = (4, 4, 8, 8, 4, 2, 1, 1)


def on_device(n, groups, wq, sq, wk, sk, wv, sv, norm_train, norm_step):
    rows, width = wq.shape
    heads = wk.shape[1]
    gain = norm_train.shape[0]
    f32, bf16 = jnp.float32, jnp.bfloat16
    shaped = jax.ShapeDtypeStruct
    me = lax.axis_index("zero").astype(jnp.int32).reshape(1)

    def swap(array, distance, axis="zero", size=n):
        return lax.ppermute(array, axis, [(i, i ^ distance) for i in range(size)])

    def gather(piece):
        found = [piece, swap(piece, 1)]
        for distance in range(2, n, 2):
            far = swap(piece, distance)
            found += [far, swap(far, 1)]
        return found

    once = lambda shape: pl.BlockSpec(shape, lambda i: (0, 0))
    full = lambda a: once(a.shape)

    columns = max(LANES, width // 8)
    place_kv = columns
    place_norm = place_kv + round_up(2 * heads, LANES)
    places = (place_kv, place_norm)
    length = place_norm + round_up(gain, LANES)
    ahead = rows * 11 // 16 // LANES * LANES
    rk, rv, early, message = pl.pallas_call(
        functools.partial(narrow_kernel, places),
        out_shape=(
            shaped((heads, rows), f32),
            shaped((heads, rows), f32),
            shaped((heads, ahead), f32),
            shaped((1, length), f32),
        ),
        in_specs=[HBM] * 8,
        out_specs=[HBM] * 4,
        scratch_shapes=[pltpu.VMEM((heads, rows), f32)] * 4
        + [pltpu.VMEM((rows, columns), f32)] * 2
        + [
            pltpu.VMEM((1, gain), f32),
            pltpu.VMEM((1, gain), f32),
            pltpu.VMEM((1, length), f32),
            pltpu.VMEM((2 * heads, LANES), f32),
            pltpu.SemaphoreType.DMA((4 * PARTS,)),
            pltpu.SemaphoreType.DMA((2 * PARTS,)),
            pltpu.SemaphoreType.DMA((2,)),
            pltpu.SemaphoreType.DMA((3 * PARTS + 1,)),
        ],
        cost_estimate=cost(rows * 2 * heads * 8, rows * 2 * heads * 16),
        name="narrow",
    )(wq, sq, wk.T, sk.T, wv.T, sv.T, norm_train[None], norm_step[None])
    messages = gather(message)
    found_early = gather(early)
    cut_a = rows * 3 // 8
    late = (heads, 2 * rows - ahead)
    own_kv, *own_a, inv_k, factor_k, factor_v, norms = pl.pallas_call(
        functools.partial(first_kernel, places, gain, n * rows),
        grid=(1,),
        out_shape=(
            shaped(late, bf16),
            shaped((cut_a, columns), bf16),
            shaped((rows - cut_a, columns), bf16),
            shaped((heads, LANES), f32),
            shaped((1, heads), f32),
            shaped((1, heads), f32),
            shaped((n, gain), f32),
        ),
        in_specs=[SMEM]
        + [full(rk)] * 2
        + [once((rows, columns))] * 2
        + [full(message)] * n,
        out_specs=[
            once(late),
            once((cut_a, columns)),
            once((rows - cut_a, columns)),
            once((heads, LANES)),
            once((1, heads)),
            once((1, heads)),
            once((n, gain)),
        ],
        cost_estimate=cost(rows * heads * 8, rows * heads * 12),
        name="first",
    )(me, rk, rv, wq, sq, *messages)
    found_kv = gather(own_kv)
    found_a = [gather(piece) for piece in own_a]

    parts = 16
    rq, message_q = pl.pallas_call(
        average_kernel,
        out_shape=(shaped((rows, width), f32), shaped((1, width), f32)),
        in_specs=[HBM] * 2,
        out_specs=[HBM] * 2,
        scratch_shapes=[pltpu.VMEM((rows, width), f32)] * 2
        + [pltpu.VMEM((1, width), f32)]
        + [pltpu.SemaphoreType.DMA((parts,))] * 3
        + [pltpu.SemaphoreType.DMA],
        cost_estimate=cost(rows * width * 8, rows * width * 12),
        name="average",
    )(wq, sq)
    messages_q = gather(message_q)

    unit = rows // sum(CUTS)
    firsts = [sum(CUTS[:at]) for at in range(len(CUTS))]
    rest = width - columns
    rows_of = lambda at: pl.BlockSpec(
        (CUTS[at] * unit, width), lambda i: (firsts[at] // CUTS[at], 0)
    )
    narrow = [shaped((c * unit, rest), bf16) for c in CUTS]
    own0, inv, factor_q = pl.pallas_call(
        functools.partial(third_kernel, columns, n * rows),
        grid=(1,),
        out_shape=(narrow[0], shaped((1, rest), f32), shaped((1, width), f32)),
        in_specs=[rows_of(0)] + [full(message_q)] * n,
        out_specs=[full(narrow[0]), once((1, rest)), once((1, width))],
        cost_estimate=cost(narrow[0].size * 8, narrow[0].size * 6),
        name="third",
    )(rq, *messages_q)
    others = range(1, len(CUTS))
    owns = pl.pallas_call(
        fourth_kernel,
        grid=(1,),
        out_shape=narrow[1:],
        in_specs=[full(inv)] + [rows_of(at) for at in others],
        out_specs=[full(narrow[at]) for at in others],
        cost_estimate=cost(rows * rest * 8, rows * rest * 6),
        name="fourth",
    )(inv, *[rq for _ in others])
    found = [gather(piece) for piece in [own0, *owns]]

    whole = shaped((n * rows, width), bf16)
    whole_kv = shaped((heads, n * rows), bf16)

    def place(jobs, final=None, extra=(), spec=None):
        pieces = [job[0] for job in jobs]
        moved = sum(p.size for p in pieces) * 2
        return pl.pallas_call(
            functools.partial(
                place_kernel,
                [job[1:] for job in jobs],
                rows,
                len(extra) + (final is not None),
            ),
            out_shape=whole,
            in_specs=[SMEM]
            + [spec or VMEM] * len(pieces)
            + [HBM] * (len(extra) + (final is not None)),
            out_specs=HBM,
            scratch_shapes=[pltpu.SemaphoreType.DMA((len(jobs),))],
            input_output_aliases={} if final is None else {1 + len(pieces): 0},
            compiler_params=leaving(54000) if spec else None,
            cost_estimate=cost(moved * 4, 2 * moved),
        )(me, *pieces, *(() if final is None else (final,)), *extra)

    def jobs(chunks, distances):
        return [
            (found[at][d], d, firsts[at] * unit, columns) for at in chunks for d in distances
        ]

    gains = norms.astype(jnp.bfloat16).reshape(n, 1, gain)
    spot = lax.axis_index("width")
    bit = 1
    while bit < groups:
        other = swap(gains, bit, "width", groups)
        low = (spot & bit) == 0
        gains = jnp.concatenate(
            [jnp.where(low, gains, other), jnp.where(low, other, gains)], axis=1
        )
        bit *= 2
    serve = gains.reshape(n * groups * gain)

    near, far = range(2), range(2, n)
    final_q = place(
        [(found_a[at][d], d, at * cut_a, 0) for at in range(2) for d in range(n)],
    )
    moved = n * own_kv.size * 2
    final_k, final_v = pl.pallas_call(
        functools.partial(place_kv_kernel, n),
        grid=(1,),
        out_shape=[whole_kv] * 2,
        in_specs=[SMEM, full(inv_k)] + [full(early)] * n + [full(own_kv)] * n,
        out_specs=[HBM] * 2,
        scratch_shapes=[
            pltpu.VMEM((n, heads, ahead), bf16),
            pltpu.SemaphoreType.DMA((3 * n,)),
        ],
        cost_estimate=cost(moved * 4, 2 * moved),
        name="place_kv",
    )(me, inv_k, *found_early, *found_kv)
    for name, chunks, distances in (
        ("place_near", range(len(CUTS)), near),
        ("place1", (0, 1), far),
        ("place2", (2,), far),
        ("place3", (3,), far),
        ("place4", (4,), far),
        ("place5", (5,), far),
        ("place6", (6, 7), far),
    ):
        extra = (serve,) if name == "place1" else ()
        spec = HBM if name in ("place5", "place6") else None
        final_q = place(jobs(chunks, distances), final_q, extra, spec)

    return (
        final_q,
        final_k.T,
        final_v.T,
        factor_q.reshape(width),
        factor_k.reshape(heads),
        factor_v.reshape(heads),
        serve,
        rq,
        rk.T,
        rv.T,
    )


def solution(mesh):
    split, columns, lone = P("zero", "width"), P(None, "width"), P("width")
    vector = P(("zero", "width"))
    n = mesh.shape["zero"]

    def body(*args):
        return on_device(n, mesh.shape["width"], *args)

    return jax.shard_map(
        body,
        mesh=mesh,
        in_specs=(split,) * 6 + (vector,) * 2,
        out_specs=(columns,) * 3 + (lone,) * 3 + (P(),) + (split,) * 3,
        check_vma=False,
    )
```

```python
import functools

import jax
import jax.numpy as jnp
from jax import lax
from jax.experimental import pallas as pl
from jax.experimental.pallas import tpu as pltpu
from jax.sharding import PartitionSpec as P


KEEP = 0.7
LANES = 128
GRANT_KIB = 60 * 1024

VMEM = pl.BlockSpec(memory_space=pltpu.VMEM)
SMEM = pl.BlockSpec(memory_space=pltpu.SMEM)
HBM = pl.BlockSpec(memory_space=pl.ANY)


def cost(flops, bytes_accessed):
    return pl.CostEstimate(flops=flops, bytes_accessed=bytes_accessed, transcendentals=0)


def leaving(kibibytes):
    return pltpu.CompilerParams(vmem_limit_bytes=(GRANT_KIB - kibibytes) << 10)


def round_up(value, step):
    return -(-value // step) * step


def average(smooth, weight):
    return KEEP * smooth + (1.0 - KEEP) * weight


def lane_sum(block):
    total = block[:, :LANES]
    for at in range(LANES, block.shape[1], LANES):
        total = total + block[:, at : at + LANES]
    return total


def row_sum(block):
    return jnp.sum(block.reshape(block.shape[0] // 8, 8, block.shape[1]), axis=0)


def load(sources, buffers, parts, sems):
    copies = []
    for at in range(parts):
        copies.append([])
        for source, buffer in zip(sources, buffers):
            step = buffer.shape[0] // parts
            rows = pl.ds(at * step, step)
            slot = sems.at[at * len(sources) + len(copies[-1])]
            copies[-1].append(
                pltpu.make_async_copy(
                    source.at[rows, pl.ds(0, buffer.shape[1])], buffer.at[rows, :], slot
                )
            )
            copies[-1][-1].start()

    def wait(at):
        for copy in copies[at]:
            copy.wait()

    return wait


PARTS = 1
PARTS_Q = 2


def narrow_kernel(places, wq, sq, wk, sk, wv, sv, nt, ns, rk, rv, early, message, *refs):
    *buffers, gain_a, gain_b, note, sum_kv, in_kv, in_q, in_gain, outs = refs
    of_kv, of_q = buffers[:4], buffers[4:]
    place_kv, place_norm = places
    heads, rows = of_kv[0].shape
    wait_kv = load((wk, sk, wv, sv), of_kv, PARTS, in_kv)
    wait_gain = load((nt, ns), (gain_a, gain_b), 1, in_gain)
    wait_q = load((wq, sq), of_q, PARTS_Q, in_q)
    step = heads // PARTS
    writes = []

    def write(source, target):
        writes.append(pltpu.make_async_copy(source, target, outs.at[len(writes)]))
        writes[-1].start()

    for part in range(PARTS):
        wait_kv(part)
        at = pl.ds(part * step, step)
        for which, (w, s, r) in enumerate(((of_kv[0], of_kv[1], rk), (of_kv[2], of_kv[3], rv))):
            new = average(s[at, :], w[at, :])
            sum_kv[which * heads + part * step : which * heads + (part + 1) * step, :] = (
                lane_sum(jnp.abs(new))
            )
            s[at, :] = new
            write(s.at[at, :], r.at[at, :])
            if which == 0:
                write(s.at[at, pl.ds(0, early.shape[1])], early.at[at, :])
    total = jnp.zeros((8, of_q[0].shape[1]), jnp.float32)
    step = rows // PARTS_Q
    for part in range(PARTS_Q):
        wait_q(part)
        at = pl.ds(part * step, step)
        total = total + row_sum(jnp.abs(average(of_q[1][at, :], of_q[0][at, :])))
    note[...] = jnp.zeros_like(note)
    note[:, : total.shape[1]] = jnp.sum(total, axis=0, keepdims=True)
    note[:, place_kv : place_kv + 2 * heads] = jnp.sum(
        sum_kv[...].T, axis=0, keepdims=True
    )
    wait_gain(0)
    gain = (gain_a[...] + gain_b[...]).astype(jnp.bfloat16)
    note[:, place_norm : place_norm + gain.shape[1]] = gain.astype(jnp.float32)
    write(note, message)
    for copy in writes:
        copy.wait()


def tree(pieces):
    while len(pieces) > 1:
        pieces = [a + b for a, b in zip(pieces[::2], pieces[1::2])]
    return pieces[0]


def first_kernel(places, heads, gain, count, me, rk, wq, sq, *refs):
    n = len(refs) - 7
    messages, (own_k, own_a, own_b, inv_k, factor_k, factor_v, norms) = refs[:n], refs[n:]
    place_kv, place_norm = places
    pieces = [m[...] for m in messages]
    for distance, piece in enumerate(pieces):
        norms[pl.ds(me[0] ^ distance, 1), :] = piece[:, place_norm : place_norm + gain]
    total = tree(pieces) / count
    scale = 1.0 / total[:, : own_a.shape[1]]
    first = 0
    for part in (own_a, own_b):
        at = pl.ds(first, part.shape[0])
        first += part.shape[0]
        part[...] = (average(sq[at, :], wq[at, :]) * scale).astype(jnp.bfloat16)
    of_kv = total[:, place_kv : place_kv + 2 * heads]
    factor_k[...] = of_kv[:, :heads]
    factor_v[...] = of_kv[:, heads:]
    inv = jnp.broadcast_to(1.0 / of_kv[:, :heads], (LANES, heads)).T
    inv_k[...] = inv
    late = own_k.shape[1]
    scale_lanes(rk, inv, own_k, rk.shape[1] - late, 0, late)


def scale_lanes(source, scale, target, first, to, count):
    for at in range(0, count, LANES):
        target[:, to + at : to + at + LANES] = (
            source[:, first + at : first + at + LANES] * scale
        ).astype(jnp.bfloat16)


def sizes_kernel(wq, sq, message, w, s, note, ins, sent):
    parts = ins.shape[0] // 2
    step = w.shape[0] // parts

    def copies(at):
        rows = pl.ds(pl.multiple_of(at * step, step), step)
        return (
            pltpu.make_async_copy(wq.at[rows, :], w.at[rows, :], ins.at[2 * at]),
            pltpu.make_async_copy(sq.at[rows, :], s.at[rows, :], ins.at[2 * at + 1]),
        )

    @pl.loop(0, parts)
    def _(at):
        for copy in copies(at):
            copy.start()

    def body(at, total):
        for copy in copies(at):
            copy.wait()
        rows = pl.ds(pl.multiple_of(at * step, step), step)
        return total + row_sum(jnp.abs(average(s[rows, :], w[rows, :])))

    total = lax.fori_loop(0, parts, body, jnp.zeros((8, w.shape[1]), jnp.float32))
    note[...] = jnp.sum(total, axis=0, keepdims=True)
    send = pltpu.make_async_copy(note, message, sent)
    send.start()
    send.wait()


def third_kernel(columns, count, wq, sq, *refs):
    messages, (own, inv, factor) = refs[:-3], refs[-3:]
    total = tree([m[...] for m in messages]) / count
    factor[...] = total
    scale = 1.0 / total[:, columns:]
    inv[...] = scale
    new = average(sq[:, columns:], wq[:, columns:])
    own[...] = (new * scale).astype(jnp.bfloat16)


def next_kernel(wq, sq, inv, own):
    columns = wq.shape[1] - own.shape[1]
    new = average(sq[:, columns:], wq[:, columns:])
    own[...] = (new * inv[...]).astype(jnp.bfloat16)


def fourth_kernel(sizes, wq, sq, inv, rq, *refs):
    owns, (w, s, scale, narrow, ins, outs) = refs[: len(sizes) - 2], refs[len(sizes) - 2 :]
    columns = w.shape[1] - narrow.shape[1]
    pieces, first = [], 0
    for chunk, size in enumerate(sizes):
        step = min(size, sizes[0] // 2)
        for at in range(0, size, step):
            pieces.append((chunk, at, first + at, step))
        first += size
    pieces = [p for p in pieces if p[0] > 1] + [p for p in pieces if p[0] < 2]
    loads, writes = [], []
    known = pltpu.make_async_copy(inv, scale, ins.at[0])
    known.start()
    for at, (_, _, row, step) in enumerate(pieces):
        rows = pl.ds(row, step)
        loads.append(
            (
                pltpu.make_async_copy(wq.at[rows, :], w.at[rows, :], ins.at[2 * at + 1]),
                pltpu.make_async_copy(sq.at[rows, :], s.at[rows, :], ins.at[2 * at + 2]),
            )
        )
        for copy in loads[-1]:
            copy.start()

    def write(source, target):
        writes.append(pltpu.make_async_copy(source, target, outs.at[len(writes)]))
        writes[-1].start()

    known.wait()
    for (chunk, at, row, step), copies in zip(pieces, loads):
        for copy in copies:
            copy.wait()
        rows = pl.ds(row, step)
        new = average(s[rows, :], w[rows, :])
        s[rows, :] = new
        write(s.at[rows, :], rq.at[rows, :])
        if chunk > 1:
            narrow[rows, :] = (new[:, columns:] * scale[...]).astype(jnp.bfloat16)
            write(narrow.at[rows, :], owns[chunk - 2].at[pl.ds(at, step), :])
    for copy in writes:
        copy.wait()


def place_kernel(plan, rows, unread, me, *refs):
    pieces, refs = refs[: len(plan)], refs[len(plan) + unread :]
    out, sems = refs
    copies = []
    for piece, (distance, first, column) in zip(pieces, plan):
        start = pl.multiple_of((me[0] ^ distance) * rows + first, 16)
        target = out.at[pl.ds(start, piece.shape[0]), pl.ds(column, piece.shape[1])]
        copies.append(pltpu.make_async_copy(piece, target, sems.at[len(copies)]))
        copies[-1].start()
    for copy in copies:
        copy.wait()


def place_kv_kernel(n, me, inv, *refs):
    early, keys, values = refs[:n], refs[n : 2 * n], refs[2 * n : 3 * n]
    out_k, out_v, scaled, sems = refs[3 * n :]
    part = early[0].shape[1]
    rows = values[0].shape[1]
    copies = []

    def move(source, target):
        copies.append(pltpu.make_async_copy(source, target, sems.at[len(copies)]))
        copies[-1].start()

    starts = [pl.multiple_of((me[0] ^ distance) * rows, LANES) for distance in range(n)]
    for start, key, value in zip(starts, keys, values):
        move(key, out_k.at[:, pl.ds(start + part, rows - part)])
        move(value, out_v.at[:, pl.ds(start, rows)])
    for distance, start in enumerate(starts):
        scale_lanes(early[distance], inv[...], scaled.at[distance], 0, 0, part)
        move(scaled.at[distance], out_k.at[:, pl.ds(start, part)])
    for copy in copies:
        copy.wait()


CUTS = (4, 4, 8, 8, 4, 2, 1, 1)
CUT_A = 6


def on_device(n, groups, wq, sq, wk, sk, wv, sv, norm_train, norm_step):
    rows, width = wq.shape
    heads = wk.shape[1]
    gain = norm_train.shape[0]
    f32, bf16 = jnp.float32, jnp.bfloat16
    shaped = jax.ShapeDtypeStruct
    me = lax.axis_index("zero").astype(jnp.int32).reshape(1)

    def swap(array, distance, axis="zero", size=n):
        return lax.ppermute(array, axis, [(i, i ^ distance) for i in range(size)])

    def gather(piece):
        found = [piece, swap(piece, 1)]
        for distance in range(2, n, 2):
            far = swap(piece, distance)
            found += [far, swap(far, 1)]
        return found

    once = lambda shape: pl.BlockSpec(shape, lambda i: (0, 0))
    full = lambda a: once(a.shape)

    columns = max(LANES, width // 4)
    place_kv = columns
    place_norm = place_kv + round_up(2 * heads, LANES)
    places = (place_kv, place_norm)
    length = place_norm + round_up(gain, LANES)
    ahead = rows * 9 // 16 // LANES * LANES
    rk, rv, early, message = pl.pallas_call(
        functools.partial(narrow_kernel, places),
        out_shape=(
            shaped((heads, rows), f32),
            shaped((heads, rows), f32),
            shaped((heads, ahead), f32),
            shaped((1, length), f32),
        ),
        in_specs=[HBM] * 8,
        out_specs=[HBM] * 4,
        scratch_shapes=[pltpu.VMEM((heads, rows), f32)] * 4
        + [pltpu.VMEM((rows, columns), f32)] * 2
        + [
            pltpu.VMEM((1, gain), f32),
            pltpu.VMEM((1, gain), f32),
            pltpu.VMEM((1, length), f32),
            pltpu.VMEM((2 * heads, LANES), f32),
            pltpu.SemaphoreType.DMA((4 * PARTS,)),
            pltpu.SemaphoreType.DMA((2 * PARTS_Q,)),
            pltpu.SemaphoreType.DMA((2,)),
            pltpu.SemaphoreType.DMA((3 * PARTS + 1,)),
        ],
        cost_estimate=cost(rows * 2 * heads * 8, rows * 2 * heads * 16),
        name="narrow",
    )(wq, sq, wk.T, sk.T, wv.T, sv.T, norm_train[None], norm_step[None])
    messages = gather(message)
    found_early = gather(early)
    total = tree(list(messages)) / (n * rows)
    of_v = total[0, place_kv + heads : place_kv + 2 * heads, None]
    own_v = (rv / of_v).astype(bf16)
    cut_a = rows * CUT_A // 16
    own_k, *own_a, inv_k, factor_k, factor_v, norms = pl.pallas_call(
        functools.partial(first_kernel, places, heads, gain, n * rows),
        grid=(1,),
        out_shape=(
            shaped((heads, rows - ahead), bf16),
            shaped((cut_a, columns), bf16),
            shaped((rows - cut_a, columns), bf16),
            shaped((heads, LANES), f32),
            shaped((1, heads), f32),
            shaped((1, heads), f32),
            shaped((n, gain), f32),
        ),
        in_specs=[SMEM, full(rk)] + [once((rows, columns))] * 2 + [full(message)] * n,
        out_specs=[
            once((heads, rows - ahead)),
            once((cut_a, columns)),
            once((rows - cut_a, columns)),
            once((heads, LANES)),
            once((1, heads)),
            once((1, heads)),
            once((n, gain)),
        ],
        cost_estimate=cost(rows * columns * 8, rows * columns * 12),
        name="first",
    )(me, rk, wq, sq, *messages)
    found_v, found_k = gather(own_v), gather(own_k)
    found_a = [gather(piece) for piece in own_a]

    parts = 8
    message_q = pl.pallas_call(
        sizes_kernel,
        out_shape=shaped((1, width), f32),
        in_specs=[HBM] * 2,
        out_specs=HBM,
        scratch_shapes=[pltpu.VMEM((rows, width), f32)] * 2
        + [pltpu.VMEM((1, width), f32)]
        + [pltpu.SemaphoreType.DMA((2 * parts,)), pltpu.SemaphoreType.DMA],
        cost_estimate=cost(rows * width * 8, rows * width * 8),
        name="sizes",
    )(wq, sq)
    messages_q = gather(message_q)

    unit = rows // sum(CUTS)
    firsts = [sum(CUTS[:at]) for at in range(len(CUTS))]
    rest = width - columns
    rows_of = lambda at: pl.BlockSpec(
        (CUTS[at] * unit, width), lambda i: (firsts[at] // CUTS[at], 0)
    )
    narrow = [shaped((c * unit, rest), bf16) for c in CUTS]
    own0, inv, factor_q = pl.pallas_call(
        functools.partial(third_kernel, columns, n * rows),
        grid=(1,),
        out_shape=(narrow[0], shaped((1, rest), f32), shaped((1, width), f32)),
        in_specs=[rows_of(0)] * 2 + [full(message_q)] * n,
        out_specs=[full(narrow[0]), once((1, rest)), once((1, width))],
        cost_estimate=cost(narrow[0].size * 8, narrow[0].size * 10),
        name="third",
    )(wq, sq, *messages_q)
    own1 = pl.pallas_call(
        next_kernel,
        grid=(1,),
        out_shape=narrow[1],
        in_specs=[rows_of(1)] * 2 + [full(inv)],
        out_specs=full(narrow[1]),
        cost_estimate=cost(narrow[1].size * 8, narrow[1].size * 10),
        name="next",
    )(wq, sq, inv)
    rq, *owns = pl.pallas_call(
        functools.partial(fourth_kernel, [c * unit for c in CUTS]),
        out_shape=[shaped((rows, width), f32)] + narrow[2:],
        in_specs=[HBM] * 3,
        out_specs=[HBM] * (len(CUTS) - 1),
        scratch_shapes=[pltpu.VMEM((rows, width), f32)] * 2
        + [pltpu.VMEM((1, rest), f32), pltpu.VMEM((rows, rest), bf16)]
        + [pltpu.SemaphoreType.DMA((65,)), pltpu.SemaphoreType.DMA((64,))],
        cost_estimate=cost(rows * width * 8, rows * width * 14),
        name="fourth",
    )(wq, sq, inv)
    found = [gather(piece) for piece in [own0, own1, *owns]]

    whole = shaped((n * rows, width), bf16)
    whole_kv = shaped((heads, n * rows), bf16)

    def place(jobs, final=None, extra=(), spec=None):
        pieces = [job[0] for job in jobs]
        moved = sum(p.size for p in pieces) * 2
        return pl.pallas_call(
            functools.partial(
                place_kernel,
                [job[1:] for job in jobs],
                rows,
                len(extra) + (final is not None),
            ),
            out_shape=whole,
            in_specs=[SMEM]
            + [spec or VMEM] * len(pieces)
            + [HBM] * (len(extra) + (final is not None)),
            out_specs=HBM,
            scratch_shapes=[pltpu.SemaphoreType.DMA((len(jobs),))],
            input_output_aliases={} if final is None else {1 + len(pieces): 0},
            compiler_params=leaving(54000) if spec else None,
            cost_estimate=cost(moved * 4, 2 * moved),
        )(me, *pieces, *(() if final is None else (final,)), *extra)

    def jobs(chunks, distances):
        return [
            (found[at][d], d, firsts[at] * unit, columns) for at in chunks for d in distances
        ]

    gains = norms.astype(jnp.bfloat16).reshape(n, 1, gain)
    spot = lax.axis_index("width")
    bit = 1
    while bit < groups:
        other = swap(gains, bit, "width", groups)
        low = (spot & bit) == 0
        gains = jnp.concatenate(
            [jnp.where(low, gains, other), jnp.where(low, other, gains)], axis=1
        )
        bit *= 2
    serve = gains.reshape(n * groups * gain)

    near, far = range(2), range(2, n)
    final_q = place([(found_a[at][d], d, at * cut_a, 0) for at in range(2) for d in range(n)])
    moved = n * own_v.size * 4
    final_k, final_v = pl.pallas_call(
        functools.partial(place_kv_kernel, n),
        grid=(1,),
        out_shape=[whole_kv] * 2,
        in_specs=[SMEM, full(inv_k)]
        + [full(early)] * n
        + [full(own_k)] * n
        + [full(own_v)] * n,
        out_specs=[HBM] * 2,
        scratch_shapes=[
            pltpu.VMEM((n, heads, ahead), bf16),
            pltpu.SemaphoreType.DMA((3 * n,)),
        ],
        cost_estimate=cost(moved * 4, 2 * moved),
        name="place_kv",
    )(me, inv_k, *found_early, *found_k, *found_v)
    for name, chunks, distances in (
        ("place_near", range(len(CUTS)), near),
        ("place1", (0, 1), far),
        ("place2", (2,), far),
        ("place3", (3,), far),
        ("place4", (4,), far),
        ("place5", (5,), far),
        ("place6", (6, 7), far),
    ):
        extra = (serve,) if name == "place1" else ()
        spec = HBM if name in ("place5", "place6") else None
        final_q = place(jobs(chunks, distances), final_q, extra, spec)

    return (
        final_q,
        final_k.T,
        final_v.T,
        factor_q.reshape(width),
        factor_k.reshape(heads),
        factor_v.reshape(heads),
        serve,
        rq,
        rk.T,
        rv.T,
    )


def solution(mesh):
    split, columns, lone = P("zero", "width"), P(None, "width"), P("width")
    vector = P(("zero", "width"))
    n = mesh.shape["zero"]

    def body(*args):
        return on_device(n, mesh.shape["width"], *args)

    return jax.shard_map(
        body,
        mesh=mesh,
        in_specs=(split,) * 6 + (vector,) * 2,
        out_specs=(columns,) * 3 + (lone,) * 3 + (P(),) + (split,) * 3,
        check_vma=False,
    )
```

```python
import functools

import jax
import jax.numpy as jnp
from jax import lax
from jax.experimental import pallas as pl
from jax.experimental.pallas import tpu as pltpu
from jax.sharding import PartitionSpec as P


KEEP = 0.7
LANES = 128
GRANT_KIB = 60 * 1024

VMEM = pl.BlockSpec(memory_space=pltpu.VMEM)
SMEM = pl.BlockSpec(memory_space=pltpu.SMEM)
HBM = pl.BlockSpec(memory_space=pl.ANY)


def cost(flops, bytes_accessed):
    return pl.CostEstimate(flops=flops, bytes_accessed=bytes_accessed, transcendentals=0)


def leaving(kibibytes):
    return pltpu.CompilerParams(vmem_limit_bytes=(GRANT_KIB - kibibytes) << 10)


def round_up(value, step):
    return -(-value // step) * step


def average(smooth, weight):
    return KEEP * smooth + (1.0 - KEEP) * weight


def lane_sum(block):
    total = block[:, :LANES]
    for at in range(LANES, block.shape[1], LANES):
        total = total + block[:, at : at + LANES]
    return total


def row_sum(block):
    return jnp.sum(block.reshape(block.shape[0] // 8, 8, block.shape[1]), axis=0)


def load(sources, buffers, parts, sems):
    copies = []
    for at in range(parts):
        copies.append([])
        for source, buffer in zip(sources, buffers):
            step = buffer.shape[0] // parts
            rows = pl.ds(at * step, step)
            slot = sems.at[at * len(sources) + len(copies[-1])]
            copies[-1].append(
                pltpu.make_async_copy(
                    source.at[rows, pl.ds(0, buffer.shape[1])], buffer.at[rows, :], slot
                )
            )
            copies[-1][-1].start()

    def wait(at):
        for copy in copies[at]:
            copy.wait()

    return wait


PARTS = 1
PARTS_Q = 2


def narrow_kernel(places, wq, sq, wk, sk, wv, sv, nt, ns, rk, rv, early, message, *refs):
    *buffers, gain_a, gain_b, note, sum_kv, in_kv, in_q, in_gain, outs = refs
    of_kv, of_q = buffers[:4], buffers[4:]
    place_kv, place_norm = places
    heads, rows = of_kv[0].shape
    wait_kv = load((wk, sk, wv, sv), of_kv, PARTS, in_kv)
    wait_gain = load((nt, ns), (gain_a, gain_b), 1, in_gain)
    wait_q = load((wq, sq), of_q, PARTS_Q, in_q)
    step = heads // PARTS
    writes = []

    def write(source, target):
        writes.append(pltpu.make_async_copy(source, target, outs.at[len(writes)]))
        writes[-1].start()

    for part in range(PARTS):
        wait_kv(part)
        at = pl.ds(part * step, step)
        for which, (w, s, r) in enumerate(((of_kv[0], of_kv[1], rk), (of_kv[2], of_kv[3], rv))):
            new = average(s[at, :], w[at, :])
            sum_kv[which * heads + part * step : which * heads + (part + 1) * step, :] = (
                lane_sum(jnp.abs(new))
            )
            s[at, :] = new
            write(s.at[at, :], r.at[at, :])
            if which == 0:
                write(s.at[at, pl.ds(0, early.shape[1])], early.at[at, :])
    total = jnp.zeros((8, of_q[0].shape[1]), jnp.float32)
    step = rows // PARTS_Q
    for part in range(PARTS_Q):
        wait_q(part)
        at = pl.ds(part * step, step)
        total = total + row_sum(jnp.abs(average(of_q[1][at, :], of_q[0][at, :])))
    note[...] = jnp.zeros_like(note)
    note[:, : total.shape[1]] = jnp.sum(total, axis=0, keepdims=True)
    note[:, place_kv : place_kv + 2 * heads] = jnp.sum(
        sum_kv[...].T, axis=0, keepdims=True
    )
    wait_gain(0)
    gain = (gain_a[...] + gain_b[...]).astype(jnp.bfloat16)
    note[:, place_norm : place_norm + gain.shape[1]] = gain.astype(jnp.float32)
    write(note, message)
    for copy in writes:
        copy.wait()


def tree(pieces):
    while len(pieces) > 1:
        pieces = [a + b for a, b in zip(pieces[::2], pieces[1::2])]
    return pieces[0]


def first_kernel(places, heads, gain, count, me, rk, wq, sq, *refs):
    n = len(refs) - 7
    messages, (own_k, own_a, own_b, inv_k, factor_k, factor_v, norms) = refs[:n], refs[n:]
    place_kv, place_norm = places
    pieces = [m[...] for m in messages]
    for distance, piece in enumerate(pieces):
        norms[pl.ds(me[0] ^ distance, 1), :] = piece[:, place_norm : place_norm + gain]
    total = tree(pieces) / count
    scale = 1.0 / total[:, : own_a.shape[1]]
    first = 0
    for part in (own_a, own_b):
        at = pl.ds(first, part.shape[0])
        first += part.shape[0]
        part[...] = (average(sq[at, :], wq[at, :]) * scale).astype(jnp.bfloat16)
    of_kv = total[:, place_kv : place_kv + 2 * heads]
    factor_k[...] = of_kv[:, :heads]
    factor_v[...] = of_kv[:, heads:]
    inv = jnp.broadcast_to(1.0 / of_kv[:, :heads], (LANES, heads)).T
    inv_k[...] = inv
    late = own_k.shape[1]
    scale_lanes(rk, inv, own_k, rk.shape[1] - late, 0, late)


def scale_lanes(source, scale, target, first, to, count):
    for at in range(0, count, LANES):
        target[:, to + at : to + at + LANES] = (
            source[:, first + at : first + at + LANES] * scale
        ).astype(jnp.bfloat16)


def sizes_kernel(wq, sq, message, w, s, note, ins, sent):
    parts = ins.shape[0] // 2
    step = w.shape[0] // parts

    def copies(at):
        rows = pl.ds(pl.multiple_of(at * step, step), step)
        return (
            pltpu.make_async_copy(wq.at[rows, :], w.at[rows, :], ins.at[2 * at]),
            pltpu.make_async_copy(sq.at[rows, :], s.at[rows, :], ins.at[2 * at + 1]),
        )

    @pl.loop(0, parts)
    def _(at):
        for copy in copies(at):
            copy.start()

    def body(at, total):
        for copy in copies(at):
            copy.wait()
        rows = pl.ds(pl.multiple_of(at * step, step), step)
        return total + row_sum(jnp.abs(average(s[rows, :], w[rows, :])))

    total = lax.fori_loop(0, parts, body, jnp.zeros((8, w.shape[1]), jnp.float32))
    note[...] = jnp.sum(total, axis=0, keepdims=True)
    send = pltpu.make_async_copy(note, message, sent)
    send.start()
    send.wait()


def third_kernel(columns, count, wq, sq, *refs):
    messages, (own, inv, factor) = refs[:-3], refs[-3:]
    total = tree([m[...] for m in messages]) / count
    factor[...] = total
    scale = 1.0 / total[:, columns:]
    inv[...] = scale
    new = average(sq[:, columns:], wq[:, columns:])
    own[...] = (new * scale).astype(jnp.bfloat16)


def next_kernel(wq, sq, inv, own):
    columns = wq.shape[1] - own.shape[1]
    new = average(sq[:, columns:], wq[:, columns:])
    own[...] = (new * inv[...]).astype(jnp.bfloat16)


def fourth_kernel(sizes, wq, sq, inv, rq, *refs):
    owns, (w, s, scale, narrow, ins, outs) = refs[: len(sizes) - 2], refs[len(sizes) - 2 :]
    columns = w.shape[1] - narrow.shape[1]
    pieces, first = [], 0
    for chunk, size in enumerate(sizes):
        step = min(size, sizes[0] // 2)
        for at in range(0, size, step):
            pieces.append((chunk, at, first + at, step))
        first += size
    pieces = [p for p in pieces if p[0] > 1] + [p for p in pieces if p[0] < 2]
    loads, writes = [], []
    known = pltpu.make_async_copy(inv, scale, ins.at[0])
    known.start()
    for at, (_, _, row, step) in enumerate(pieces):
        rows = pl.ds(row, step)
        loads.append(
            (
                pltpu.make_async_copy(wq.at[rows, :], w.at[rows, :], ins.at[2 * at + 1]),
                pltpu.make_async_copy(sq.at[rows, :], s.at[rows, :], ins.at[2 * at + 2]),
            )
        )
        for copy in loads[-1]:
            copy.start()

    def write(source, target):
        writes.append(pltpu.make_async_copy(source, target, outs.at[len(writes)]))
        writes[-1].start()

    known.wait()
    for (chunk, at, row, step), copies in zip(pieces, loads):
        for copy in copies:
            copy.wait()
        rows = pl.ds(row, step)
        new = average(s[rows, :], w[rows, :])
        s[rows, :] = new
        write(s.at[rows, :], rq.at[rows, :])
        if chunk > 1:
            narrow[rows, :] = (new[:, columns:] * scale[...]).astype(jnp.bfloat16)
            write(narrow.at[rows, :], owns[chunk - 2].at[pl.ds(at, step), :])
    for copy in writes:
        copy.wait()


def place_kernel(plan, rows, unread, me, *refs):
    pieces, refs = refs[: len(plan)], refs[len(plan) + unread :]
    out, sems = refs
    copies = []
    for piece, (distance, first, column) in zip(pieces, plan):
        start = pl.multiple_of((me[0] ^ distance) * rows + first, 16)
        target = out.at[pl.ds(start, piece.shape[0]), pl.ds(column, piece.shape[1])]
        copies.append(pltpu.make_async_copy(piece, target, sems.at[len(copies)]))
        copies[-1].start()
    for copy in copies:
        copy.wait()


def place_kv_kernel(n, me, inv, *refs):
    early, keys, values = refs[:n], refs[n : 2 * n], refs[2 * n : 3 * n]
    out_k, out_v, scaled, sems = refs[3 * n :]
    part = early[0].shape[1]
    rows = values[0].shape[1]
    copies = []

    def move(source, target):
        copies.append(pltpu.make_async_copy(source, target, sems.at[len(copies)]))
        copies[-1].start()

    starts = [pl.multiple_of((me[0] ^ distance) * rows, LANES) for distance in range(n)]
    for start, key, value in zip(starts, keys, values):
        move(key, out_k.at[:, pl.ds(start + part, rows - part)])
        move(value, out_v.at[:, pl.ds(start, rows)])
    for distance, start in enumerate(starts):
        scale_lanes(early[distance], inv[...], scaled.at[distance], 0, 0, part)
        move(scaled.at[distance], out_k.at[:, pl.ds(start, part)])
    for copy in copies:
        copy.wait()


CHUNKS = 7


def chunk_rows(rows):
    part = rows // 8
    return (part, part, 3 * part, 2 * part, part // 2, part // 2 - 16, 16)


CUT_A = 6


def on_device(n, groups, wq, sq, wk, sk, wv, sv, norm_train, norm_step):
    rows, width = wq.shape
    heads = wk.shape[1]
    gain = norm_train.shape[0]
    f32, bf16 = jnp.float32, jnp.bfloat16
    shaped = jax.ShapeDtypeStruct
    me = lax.axis_index("zero").astype(jnp.int32).reshape(1)

    def swap(array, distance, axis="zero", size=n):
        return lax.ppermute(array, axis, [(i, i ^ distance) for i in range(size)])

    def gather(piece, direct=False):
        found = [piece, swap(piece, 1)]
        for distance in range(2, n, 2):
            far = swap(piece, distance)
            if direct:
                found += [far, swap(piece, distance + 1)]
                continue
            found += [far, swap(far, 1)]
        return found

    once = lambda shape: pl.BlockSpec(shape, lambda i: (0, 0))
    full = lambda a: once(a.shape)

    columns = max(LANES, width // 4)
    place_kv = columns
    place_norm = place_kv + round_up(2 * heads, LANES)
    places = (place_kv, place_norm)
    length = place_norm + round_up(gain, LANES)
    ahead = rows * 9 // 16 // LANES * LANES
    rk, rv, early, message = pl.pallas_call(
        functools.partial(narrow_kernel, places),
        out_shape=(
            shaped((heads, rows), f32),
            shaped((heads, rows), f32),
            shaped((heads, ahead), f32),
            shaped((1, length), f32),
        ),
        in_specs=[HBM] * 8,
        out_specs=[HBM] * 4,
        scratch_shapes=[pltpu.VMEM((heads, rows), f32)] * 4
        + [pltpu.VMEM((rows, columns), f32)] * 2
        + [
            pltpu.VMEM((1, gain), f32),
            pltpu.VMEM((1, gain), f32),
            pltpu.VMEM((1, length), f32),
            pltpu.VMEM((2 * heads, LANES), f32),
            pltpu.SemaphoreType.DMA((4 * PARTS,)),
            pltpu.SemaphoreType.DMA((2 * PARTS_Q,)),
            pltpu.SemaphoreType.DMA((2,)),
            pltpu.SemaphoreType.DMA((3 * PARTS + 1,)),
        ],
        cost_estimate=cost(rows * 2 * heads * 8, rows * 2 * heads * 16),
        name="narrow",
    )(wq, sq, wk.T, sk.T, wv.T, sv.T, norm_train[None], norm_step[None])
    messages = gather(message)
    found_early = gather(early)
    total = tree(list(messages)) / (n * rows)
    of_v = total[0, place_kv + heads : place_kv + 2 * heads, None]
    own_v = (rv / of_v).astype(bf16)
    cut_a = rows * CUT_A // 16
    own_k, *own_a, inv_k, factor_k, factor_v, norms = pl.pallas_call(
        functools.partial(first_kernel, places, heads, gain, n * rows),
        grid=(1,),
        out_shape=(
            shaped((heads, rows - ahead), bf16),
            shaped((cut_a, columns), bf16),
            shaped((rows - cut_a, columns), bf16),
            shaped((heads, LANES), f32),
            shaped((1, heads), f32),
            shaped((1, heads), f32),
            shaped((n, gain), f32),
        ),
        in_specs=[SMEM, full(rk)] + [once((rows, columns))] * 2 + [full(message)] * n,
        out_specs=[
            once((heads, rows - ahead)),
            once((cut_a, columns)),
            once((rows - cut_a, columns)),
            once((heads, LANES)),
            once((1, heads)),
            once((1, heads)),
            once((n, gain)),
        ],
        cost_estimate=cost(rows * columns * 8, rows * columns * 12),
        name="first",
    )(me, rk, wq, sq, *messages)
    found_v, found_k = gather(own_v), gather(own_k)
    found_a = [gather(piece) for piece in own_a]

    parts = 8
    message_q = pl.pallas_call(
        sizes_kernel,
        out_shape=shaped((1, width), f32),
        in_specs=[HBM] * 2,
        out_specs=HBM,
        scratch_shapes=[pltpu.VMEM((rows, width), f32)] * 2
        + [pltpu.VMEM((1, width), f32)]
        + [pltpu.SemaphoreType.DMA((2 * parts,)), pltpu.SemaphoreType.DMA],
        cost_estimate=cost(rows * width * 8, rows * width * 8),
        name="sizes",
    )(wq, sq)
    messages_q = gather(message_q)

    sizes = chunk_rows(rows)
    firsts = [sum(sizes[:at]) for at in range(CHUNKS)]
    rest = width - columns
    rows_of = lambda at: pl.BlockSpec(
        (sizes[at], width), lambda i: (firsts[at] // sizes[at], 0)
    )
    narrow = [shaped((c, rest), bf16) for c in sizes]
    own0, inv, factor_q = pl.pallas_call(
        functools.partial(third_kernel, columns, n * rows),
        grid=(1,),
        out_shape=(narrow[0], shaped((1, rest), f32), shaped((1, width), f32)),
        in_specs=[rows_of(0)] * 2 + [full(message_q)] * n,
        out_specs=[full(narrow[0]), once((1, rest)), once((1, width))],
        cost_estimate=cost(narrow[0].size * 8, narrow[0].size * 10),
        name="third",
    )(wq, sq, *messages_q)
    own1 = pl.pallas_call(
        next_kernel,
        grid=(1,),
        out_shape=narrow[1],
        in_specs=[rows_of(1)] * 2 + [full(inv)],
        out_specs=full(narrow[1]),
        cost_estimate=cost(narrow[1].size * 8, narrow[1].size * 10),
        name="next",
    )(wq, sq, inv)
    rq, *owns = pl.pallas_call(
        functools.partial(fourth_kernel, sizes),
        out_shape=[shaped((rows, width), f32)] + narrow[2:],
        in_specs=[HBM] * 3,
        out_specs=[HBM] * (CHUNKS - 1),
        scratch_shapes=[pltpu.VMEM((rows, width), f32)] * 2
        + [pltpu.VMEM((1, rest), f32), pltpu.VMEM((rows, rest), bf16)]
        + [pltpu.SemaphoreType.DMA((65,)), pltpu.SemaphoreType.DMA((64,))],
        cost_estimate=cost(rows * width * 8, rows * width * 14),
        name="fourth",
    )(wq, sq, inv)
    found = [gather(piece) for piece in [own0, own1, *owns[:-1]]]
    found.append(gather(owns[-1], direct=True))

    whole = shaped((n * rows, width), bf16)
    whole_kv = shaped((heads, n * rows), bf16)

    def place(jobs, final=None, extra=(), spec=None):
        pieces = [job[0] for job in jobs]
        moved = sum(p.size for p in pieces) * 2
        return pl.pallas_call(
            functools.partial(
                place_kernel,
                [job[1:] for job in jobs],
                rows,
                len(extra) + (final is not None),
            ),
            out_shape=whole,
            in_specs=[SMEM]
            + [spec or VMEM] * len(pieces)
            + [HBM] * (len(extra) + (final is not None)),
            out_specs=HBM,
            scratch_shapes=[pltpu.SemaphoreType.DMA((len(jobs),))],
            input_output_aliases={} if final is None else {1 + len(pieces): 0},
            compiler_params=leaving(54000) if spec else None,
            cost_estimate=cost(moved * 4, 2 * moved),
        )(me, *pieces, *(() if final is None else (final,)), *extra)

    def jobs(chunks, distances):
        return [
            (found[at][d], d, firsts[at], columns) for at in chunks for d in distances
        ]

    gains = norms.astype(jnp.bfloat16).reshape(n, 1, gain)
    spot = lax.axis_index("width")
    bit = 1
    while bit < groups:
        other = swap(gains, bit, "width", groups)
        low = (spot & bit) == 0
        gains = jnp.concatenate(
            [jnp.where(low, gains, other), jnp.where(low, other, gains)], axis=1
        )
        bit *= 2
    serve = gains.reshape(n * groups * gain)

    near, far = range(2), range(2, n)
    final_q = place([(found_a[at][d], d, at * cut_a, 0) for at in range(2) for d in range(n)])
    moved = n * own_v.size * 4
    final_k, final_v = pl.pallas_call(
        functools.partial(place_kv_kernel, n),
        grid=(1,),
        out_shape=[whole_kv] * 2,
        in_specs=[SMEM, full(inv_k)]
        + [full(early)] * n
        + [full(own_k)] * n
        + [full(own_v)] * n,
        out_specs=[HBM] * 2,
        scratch_shapes=[
            pltpu.VMEM((n, heads, ahead), bf16),
            pltpu.SemaphoreType.DMA((3 * n,)),
        ],
        cost_estimate=cost(moved * 4, 2 * moved),
        name="place_kv",
    )(me, inv_k, *found_early, *found_k, *found_v)
    for name, chunks, distances in (
        ("place_near", range(CHUNKS), near),
        ("place1", (0, 1), far),
        ("place2", (2,), far),
        ("place3", (3,), far),
        ("place4", (4,), far),
        ("place5", (5, 6), far),
    ):
        extra = (serve,) if name == "place1" else ()
        spec = HBM if name in ("place4", "place5") else None
        final_q = place(jobs(chunks, distances), final_q, extra, spec)

    return (
        final_q,
        final_k.T,
        final_v.T,
        factor_q.reshape(width),
        factor_k.reshape(heads),
        factor_v.reshape(heads),
        serve,
        rq,
        rk.T,
        rv.T,
    )


def solution(mesh):
    split, columns, lone = P("zero", "width"), P(None, "width"), P("width")
    vector = P(("zero", "width"))
    n = mesh.shape["zero"]

    def body(*args):
        return on_device(n, mesh.shape["width"], *args)

    return jax.shard_map(
        body,
        mesh=mesh,
        in_specs=(split,) * 6 + (vector,) * 2,
        out_specs=(columns,) * 3 + (lone,) * 3 + (P(),) + (split,) * 3,
        check_vma=False,
    )
```

```python
import functools

import jax
import jax.numpy as jnp
from jax import lax
from jax.experimental import pallas as pl
from jax.experimental.pallas import tpu as pltpu
from jax.sharding import PartitionSpec as P


KEEP = 0.7
LANES = 128
GRANT_KIB = 60 * 1024

VMEM = pl.BlockSpec(memory_space=pltpu.VMEM)
SMEM = pl.BlockSpec(memory_space=pltpu.SMEM)
HBM = pl.BlockSpec(memory_space=pl.ANY)


def cost(flops, bytes_accessed):
    return pl.CostEstimate(flops=flops, bytes_accessed=bytes_accessed, transcendentals=0)


def leaving(kibibytes):
    return pltpu.CompilerParams(vmem_limit_bytes=(GRANT_KIB - kibibytes) << 10)


def round_up(value, step):
    return -(-value // step) * step


def average(smooth, weight):
    return KEEP * smooth + (1.0 - KEEP) * weight


def lane_sum(block):
    total = block[:, :LANES]
    for at in range(LANES, block.shape[1], LANES):
        total = total + block[:, at : at + LANES]
    return total


def row_sum(block):
    return jnp.sum(block.reshape(block.shape[0] // 8, 8, block.shape[1]), axis=0)


def load(sources, buffers, parts, sems):
    copies = []
    for at in range(parts):
        copies.append([])
        for source, buffer in zip(sources, buffers):
            step = buffer.shape[0] // parts
            rows = pl.ds(at * step, step)
            slot = sems.at[at * len(sources) + len(copies[-1])]
            copies[-1].append(
                pltpu.make_async_copy(
                    source.at[rows, pl.ds(0, buffer.shape[1])], buffer.at[rows, :], slot
                )
            )
            copies[-1][-1].start()

    def wait(at):
        for copy in copies[at]:
            copy.wait()

    return wait


PARTS = 1
PARTS_Q = 2


def narrow_kernel(places, wq, sq, wk, sk, wv, sv, nt, ns, early, message, *refs):
    *buffers, gain_a, gain_b, note, sum_kv, in_kv, in_q, in_gain, outs = refs
    of_kv, of_q = buffers[:4], buffers[4:]
    place_kv, place_norm = places
    heads, rows = of_kv[0].shape
    wait_kv = load((wk, sk, wv, sv), of_kv, PARTS, in_kv)
    wait_gain = load((nt, ns), (gain_a, gain_b), 1, in_gain)
    wait_q = load((wq, sq), of_q, PARTS_Q, in_q)
    step = heads // PARTS
    writes = []

    def write(source, target):
        writes.append(pltpu.make_async_copy(source, target, outs.at[len(writes)]))
        writes[-1].start()

    for part in range(PARTS):
        wait_kv(part)
        at = pl.ds(part * step, step)
        for which, (w, s) in enumerate((of_kv[:2], of_kv[2:])):
            new = average(s[at, :], w[at, :])
            sum_kv[which * heads + part * step : which * heads + (part + 1) * step, :] = (
                lane_sum(jnp.abs(new))
            )
            if which == 0:
                s[at, pl.ds(0, early.shape[1])] = new[:, : early.shape[1]]
                write(s.at[at, pl.ds(0, early.shape[1])], early.at[at, :])
    total = jnp.zeros((8, of_q[0].shape[1]), jnp.float32)
    step = rows // PARTS_Q
    for part in range(PARTS_Q):
        wait_q(part)
        at = pl.ds(part * step, step)
        total = total + row_sum(jnp.abs(average(of_q[1][at, :], of_q[0][at, :])))
    note[...] = jnp.zeros_like(note)
    note[:, : total.shape[1]] = jnp.sum(total, axis=0, keepdims=True)
    note[:, place_kv : place_kv + 2 * heads] = jnp.sum(
        sum_kv[...].T, axis=0, keepdims=True
    )
    wait_gain(0)
    gain = (gain_a[...] + gain_b[...]).astype(jnp.bfloat16)
    note[:, place_norm : place_norm + gain.shape[1]] = gain.astype(jnp.float32)
    write(note, message)
    for copy in writes:
        copy.wait()


def tree(pieces):
    while len(pieces) > 1:
        pieces = [a + b for a, b in zip(pieces[::2], pieces[1::2])]
    return pieces[0]


def first_kernel(places, heads, gain, count, me, wk, sk, wv, sv, wq, sq, *refs):
    n = len(refs) - 9
    messages, outs = refs[:n], refs[n:]
    rk, rv, own_k, own_a, own_b, inv_k, factor_k, factor_v, norms = outs
    rk[...] = average(sk[...], wk[...])
    rv[...] = average(sv[...], wv[...])
    place_kv, place_norm = places
    pieces = [m[...] for m in messages]
    for distance, piece in enumerate(pieces):
        norms[pl.ds(me[0] ^ distance, 1), :] = piece[:, place_norm : place_norm + gain]
    total = tree(pieces) / count
    scale = 1.0 / total[:, : own_a.shape[1]]
    first = 0
    for part in (own_a, own_b):
        at = pl.ds(first, part.shape[0])
        first += part.shape[0]
        part[...] = (average(sq[at, :], wq[at, :]) * scale).astype(jnp.bfloat16)
    of_kv = total[:, place_kv : place_kv + 2 * heads]
    factor_k[...] = of_kv[:, :heads]
    factor_v[...] = of_kv[:, heads:]
    inv = jnp.broadcast_to(1.0 / of_kv[:, :heads], (LANES, heads)).T
    inv_k[...] = inv
    late = own_k.shape[1]
    scale_lanes(rk, inv, own_k, rk.shape[1] - late, 0, late)


def scale_lanes(source, scale, target, first, to, count):
    for at in range(0, count, LANES):
        target[:, to + at : to + at + LANES] = (
            source[:, first + at : first + at + LANES] * scale
        ).astype(jnp.bfloat16)


def sizes_kernel(wq, sq, message, w, s, note, ins, sent):
    parts = ins.shape[0] // 2
    step = w.shape[0] // parts

    def copies(at):
        rows = pl.ds(pl.multiple_of(at * step, step), step)
        return (
            pltpu.make_async_copy(wq.at[rows, :], w.at[rows, :], ins.at[2 * at]),
            pltpu.make_async_copy(sq.at[rows, :], s.at[rows, :], ins.at[2 * at + 1]),
        )

    @pl.loop(0, parts)
    def _(at):
        for copy in copies(at):
            copy.start()

    def body(at, total):
        for copy in copies(at):
            copy.wait()
        rows = pl.ds(pl.multiple_of(at * step, step), step)
        return total + row_sum(jnp.abs(average(s[rows, :], w[rows, :])))

    total = lax.fori_loop(0, parts, body, jnp.zeros((8, w.shape[1]), jnp.float32))
    note[...] = jnp.sum(total, axis=0, keepdims=True)
    send = pltpu.make_async_copy(note, message, sent)
    send.start()
    send.wait()


def third_kernel(columns, count, wq, sq, *refs):
    messages, (own, inv, factor) = refs[:-3], refs[-3:]
    total = tree([m[...] for m in messages]) / count
    factor[...] = total
    scale = 1.0 / total[:, columns:]
    inv[...] = scale
    new = average(sq[:, columns:], wq[:, columns:])
    own[...] = (new * scale).astype(jnp.bfloat16)


def next_kernel(wq, sq, inv, own):
    columns = wq.shape[1] - own.shape[1]
    new = average(sq[:, columns:], wq[:, columns:])
    own[...] = (new * inv[...]).astype(jnp.bfloat16)


def fourth_kernel(sizes, wq, sq, inv, rq, *refs):
    owns, (w, s, scale, narrow, ins, outs) = refs[: len(sizes) - 2], refs[len(sizes) - 2 :]
    columns = w.shape[1] - narrow.shape[1]
    pieces, first = [], 0
    for chunk, size in enumerate(sizes):
        step = min(size, sizes[0] // 2)
        for at in range(0, size, step):
            pieces.append((chunk, at, first + at, step))
        first += size
    pieces = [p for p in pieces if p[0] > 1] + [p for p in pieces if p[0] < 2]
    loads, writes = [], []
    known = pltpu.make_async_copy(inv, scale, ins.at[0])
    known.start()
    for at, (_, _, row, step) in enumerate(pieces):
        rows = pl.ds(row, step)
        loads.append(
            (
                pltpu.make_async_copy(wq.at[rows, :], w.at[rows, :], ins.at[2 * at + 1]),
                pltpu.make_async_copy(sq.at[rows, :], s.at[rows, :], ins.at[2 * at + 2]),
            )
        )
        for copy in loads[-1]:
            copy.start()

    def write(source, target):
        writes.append(pltpu.make_async_copy(source, target, outs.at[len(writes)]))
        writes[-1].start()

    known.wait()
    for (chunk, at, row, step), copies in zip(pieces, loads):
        for copy in copies:
            copy.wait()
        rows = pl.ds(row, step)
        new = average(s[rows, :], w[rows, :])
        s[rows, :] = new
        write(s.at[rows, :], rq.at[rows, :])
        if chunk > 1:
            narrow[rows, :] = (new[:, columns:] * scale[...]).astype(jnp.bfloat16)
            write(narrow.at[rows, :], owns[chunk - 2].at[pl.ds(at, step), :])
    for copy in writes:
        copy.wait()


def place_kernel(plan, rows, unread, me, *refs):
    pieces, refs = refs[: len(plan)], refs[len(plan) + unread :]
    out, sems = refs
    copies = []
    for piece, (distance, first, column) in zip(pieces, plan):
        start = pl.multiple_of((me[0] ^ distance) * rows + first, 16)
        target = out.at[pl.ds(start, piece.shape[0]), pl.ds(column, piece.shape[1])]
        copies.append(pltpu.make_async_copy(piece, target, sems.at[len(copies)]))
        copies[-1].start()
    for copy in copies:
        copy.wait()


def place_kv_kernel(n, me, inv, *refs):
    early, keys, values = refs[:n], refs[n : 2 * n], refs[2 * n : 3 * n]
    out_k, out_v, scaled, sems = refs[3 * n :]
    part = early[0].shape[1]
    rows = values[0].shape[1]
    copies = []

    def move(source, target):
        copies.append(pltpu.make_async_copy(source, target, sems.at[len(copies)]))
        copies[-1].start()

    starts = [pl.multiple_of((me[0] ^ distance) * rows, LANES) for distance in range(n)]
    for start, key, value in zip(starts, keys, values):
        move(key, out_k.at[:, pl.ds(start + part, rows - part)])
        move(value, out_v.at[:, pl.ds(start, rows)])
    for distance, start in enumerate(starts):
        scale_lanes(early[distance], inv[...], scaled.at[distance], 0, 0, part)
        move(scaled.at[distance], out_k.at[:, pl.ds(start, part)])
    for copy in copies:
        copy.wait()


CHUNKS = 7


def chunk_rows(rows):
    part = rows // 8
    return (part, part, 3 * part, 2 * part, part // 2, part // 2 - 16, 16)


CUT_A = 6


def on_device(n, groups, wq, sq, wk, sk, wv, sv, norm_train, norm_step):
    rows, width = wq.shape
    heads = wk.shape[1]
    gain = norm_train.shape[0]
    f32, bf16 = jnp.float32, jnp.bfloat16
    shaped = jax.ShapeDtypeStruct
    me = lax.axis_index("zero").astype(jnp.int32).reshape(1)

    def swap(array, distance, axis="zero", size=n):
        return lax.ppermute(array, axis, [(i, i ^ distance) for i in range(size)])

    def gather(piece, direct=False):
        found = [piece, swap(piece, 1)]
        for distance in range(2, n, 2):
            far = swap(piece, distance)
            if direct:
                found += [far, swap(piece, distance + 1)]
                continue
            found += [far, swap(far, 1)]
        return found

    once = lambda shape: pl.BlockSpec(shape, lambda i: (0, 0))
    full = lambda a: once(a.shape)

    columns = max(LANES, width // 4)
    place_kv = columns
    place_norm = place_kv + round_up(2 * heads, LANES)
    places = (place_kv, place_norm)
    length = place_norm + round_up(gain, LANES)
    ahead = rows * 8 // 16 // LANES * LANES
    early, message = pl.pallas_call(
        functools.partial(narrow_kernel, places),
        out_shape=(
            shaped((heads, ahead), f32),
            shaped((1, length), f32),
        ),
        in_specs=[HBM] * 8,
        out_specs=[HBM] * 2,
        scratch_shapes=[pltpu.VMEM((heads, rows), f32)] * 4
        + [pltpu.VMEM((rows, columns), f32)] * 2
        + [
            pltpu.VMEM((1, gain), f32),
            pltpu.VMEM((1, gain), f32),
            pltpu.VMEM((1, length), f32),
            pltpu.VMEM((2 * heads, LANES), f32),
            pltpu.SemaphoreType.DMA((4 * PARTS,)),
            pltpu.SemaphoreType.DMA((2 * PARTS_Q,)),
            pltpu.SemaphoreType.DMA((2,)),
            pltpu.SemaphoreType.DMA((3 * PARTS + 1,)),
        ],
        cost_estimate=cost(rows * 2 * heads * 8, rows * 2 * heads * 16),
        name="narrow",
    )(wq, sq, wk.T, sk.T, wv.T, sv.T, norm_train[None], norm_step[None])
    messages = gather(message)
    found_early = gather(early)
    total = tree(list(messages)) / (n * rows)
    of_v = total[0, place_kv + heads : place_kv + 2 * heads, None]
    own_v = (average(sv.T, wv.T) / of_v).astype(bf16)
    cut_a = rows * CUT_A // 16
    rk, rv, own_k, *own_a, inv_k, factor_k, factor_v, norms = pl.pallas_call(
        functools.partial(first_kernel, places, heads, gain, n * rows),
        grid=(1,),
        out_shape=(
            shaped((heads, rows), f32),
            shaped((heads, rows), f32),
            shaped((heads, rows - ahead), bf16),
            shaped((cut_a, columns), bf16),
            shaped((rows - cut_a, columns), bf16),
            shaped((heads, LANES), f32),
            shaped((1, heads), f32),
            shaped((1, heads), f32),
            shaped((n, gain), f32),
        ),
        in_specs=[SMEM]
        + [once((heads, rows))] * 4
        + [once((rows, columns))] * 2
        + [full(message)] * n,
        out_specs=[
            once((heads, rows)),
            once((heads, rows)),
            once((heads, rows - ahead)),
            once((cut_a, columns)),
            once((rows - cut_a, columns)),
            once((heads, LANES)),
            once((1, heads)),
            once((1, heads)),
            once((n, gain)),
        ],
        cost_estimate=cost(rows * columns * 8, rows * columns * 12),
        name="first",
    )(me, wk.T, sk.T, wv.T, sv.T, wq, sq, *messages)
    found_v, found_k = gather(own_v), gather(own_k)
    found_a = [gather(piece) for piece in own_a]

    parts = 8
    message_q = pl.pallas_call(
        sizes_kernel,
        out_shape=shaped((1, width), f32),
        in_specs=[HBM] * 2,
        out_specs=HBM,
        scratch_shapes=[pltpu.VMEM((rows, width), f32)] * 2
        + [pltpu.VMEM((1, width), f32)]
        + [pltpu.SemaphoreType.DMA((2 * parts,)), pltpu.SemaphoreType.DMA],
        cost_estimate=cost(rows * width * 8, rows * width * 8),
        name="sizes",
    )(wq, sq)
    messages_q = gather(message_q)

    sizes = chunk_rows(rows)
    firsts = [sum(sizes[:at]) for at in range(CHUNKS)]
    rest = width - columns
    rows_of = lambda at: pl.BlockSpec(
        (sizes[at], width), lambda i: (firsts[at] // sizes[at], 0)
    )
    narrow = [shaped((c, rest), bf16) for c in sizes]
    own0, inv, factor_q = pl.pallas_call(
        functools.partial(third_kernel, columns, n * rows),
        grid=(1,),
        out_shape=(narrow[0], shaped((1, rest), f32), shaped((1, width), f32)),
        in_specs=[rows_of(0)] * 2 + [full(message_q)] * n,
        out_specs=[full(narrow[0]), once((1, rest)), once((1, width))],
        cost_estimate=cost(narrow[0].size * 8, narrow[0].size * 10),
        name="third",
    )(wq, sq, *messages_q)
    own1 = pl.pallas_call(
        next_kernel,
        grid=(1,),
        out_shape=narrow[1],
        in_specs=[rows_of(1)] * 2 + [full(inv)],
        out_specs=full(narrow[1]),
        cost_estimate=cost(narrow[1].size * 8, narrow[1].size * 10),
        name="next",
    )(wq, sq, inv)
    rq, *owns = pl.pallas_call(
        functools.partial(fourth_kernel, sizes),
        out_shape=[shaped((rows, width), f32)] + narrow[2:],
        in_specs=[HBM] * 3,
        out_specs=[HBM] * (CHUNKS - 1),
        scratch_shapes=[pltpu.VMEM((rows, width), f32)] * 2
        + [pltpu.VMEM((1, rest), f32), pltpu.VMEM((rows, rest), bf16)]
        + [pltpu.SemaphoreType.DMA((65,)), pltpu.SemaphoreType.DMA((64,))],
        cost_estimate=cost(rows * width * 8, rows * width * 14),
        name="fourth",
    )(wq, sq, inv)
    found = [gather(piece) for piece in [own0, own1, *owns[:-1]]]
    found.append(gather(owns[-1], direct=True))

    whole = shaped((n * rows, width), bf16)
    whole_kv = shaped((heads, n * rows), bf16)

    def place(jobs, final=None, extra=(), spec=None):
        pieces = [job[0] for job in jobs]
        moved = sum(p.size for p in pieces) * 2
        return pl.pallas_call(
            functools.partial(
                place_kernel,
                [job[1:] for job in jobs],
                rows,
                len(extra) + (final is not None),
            ),
            out_shape=whole,
            in_specs=[SMEM]
            + [spec or VMEM] * len(pieces)
            + [HBM] * (len(extra) + (final is not None)),
            out_specs=HBM,
            scratch_shapes=[pltpu.SemaphoreType.DMA((len(jobs),))],
            input_output_aliases={} if final is None else {1 + len(pieces): 0},
            compiler_params=leaving(54000) if spec else None,
            cost_estimate=cost(moved * 4, 2 * moved),
        )(me, *pieces, *(() if final is None else (final,)), *extra)

    def jobs(chunks, distances):
        return [
            (found[at][d], d, firsts[at], columns) for at in chunks for d in distances
        ]

    gains = norms.astype(jnp.bfloat16).reshape(n, 1, gain)
    spot = lax.axis_index("width")
    bit = 1
    while bit < groups:
        other = swap(gains, bit, "width", groups)
        low = (spot & bit) == 0
        gains = jnp.concatenate(
            [jnp.where(low, gains, other), jnp.where(low, other, gains)], axis=1
        )
        bit *= 2
    serve = gains.reshape(n * groups * gain)

    near, far = range(2), range(2, n)
    final_q = place([(found_a[at][d], d, at * cut_a, 0) for at in range(2) for d in range(n)])
    moved = n * own_v.size * 4
    final_k, final_v = pl.pallas_call(
        functools.partial(place_kv_kernel, n),
        grid=(1,),
        out_shape=[whole_kv] * 2,
        in_specs=[SMEM, full(inv_k)]
        + [full(early)] * n
        + [full(own_k)] * n
        + [full(own_v)] * n,
        out_specs=[HBM] * 2,
        scratch_shapes=[
            pltpu.VMEM((n, heads, ahead), bf16),
            pltpu.SemaphoreType.DMA((3 * n,)),
        ],
        cost_estimate=cost(moved * 4, 2 * moved),
        name="place_kv",
    )(me, inv_k, *found_early, *found_k, *found_v)
    for name, chunks, distances in (
        ("place_near", range(CHUNKS), near),
        ("place1", (0, 1), far),
        ("place2", (2,), far),
        ("place3", (3,), far),
        ("place4", (4,), far),
        ("place5", (5, 6), far),
    ):
        extra = (serve,) if name == "place1" else ()
        spec = HBM if name in ("place4", "place5") else None
        final_q = place(jobs(chunks, distances), final_q, extra, spec)

    return (
        final_q,
        final_k.T,
        final_v.T,
        factor_q.reshape(width),
        factor_k.reshape(heads),
        factor_v.reshape(heads),
        serve,
        rq,
        rk.T,
        rv.T,
    )


def solution(mesh):
    split, columns, lone = P("zero", "width"), P(None, "width"), P("width")
    vector = P(("zero", "width"))
    n = mesh.shape["zero"]

    def body(*args):
        return on_device(n, mesh.shape["width"], *args)

    return jax.shard_map(
        body,
        mesh=mesh,
        in_specs=(split,) * 6 + (vector,) * 2,
        out_specs=(columns,) * 3 + (lone,) * 3 + (P(),) + (split,) * 3,
        check_vma=False,
    )
```
